128 devices in a mesh: gx: 64 (over z, y, x), gy: 2 (over core).
Axes of the slice: x: 4, y: 4, z: 4, core: 2. Of those that a mesh axis runs over, the one named last changes fastest.
Arguments:
- history: bfloat16 [512, 2048, 256], P(('gx', 'gy')), may hold values from -100 to 100
- lengths: int32 [512], P(('gx', 'gy')), may hold values from 16 to 2048
- candidates: int32 [512, 64], P(('gx', 'gy')), may hold values from 0 to 524287, as said below
- item_table: bfloat16 [524288, 512], P(('gx', 'gy')), may hold values from -6 to 6
- value_weight: bfloat16 [256, 256], replicated, may hold values from -0.375 to 0.375
- click_hidden: bfloat16 [768, 256], replicated, may hold values from -0.21875 to 0.21875
- convert_hidden: bfloat16 [768, 256], replicated, may hold values from -0.21875 to 0.21875
- click_output: bfloat16 [256], replicated, may hold values from -0.75 to 0.75
- convert_output: bfloat16 [256], replicated, may hold values from -0.75 to 0.75
Outputs:
- click_rate: float32 [512, 64], P(('gx', 'gy'))
- click_conversion: float32 [512, 64], P(('gx', 'gy'))
The draws below stay inside these ranges and needn't reach their ends.
Inputs may be any that keep to these rules, and one draw needn't show every extreme that they name: Device k holds the table rows k * 4096 to (k + 1) * 4096 - 1. Of the 256 candidates of one device, at most 4 are items of one device's rows, and exactly 4 are items of some device's rows.
All inputs are finite; a program needn't handle non-finite values.
Results may differ from the reference program's by a relative error of at most 0.0028.
Values may be sent and summed in bfloat16 or wider, within the bound.
No kernel may reach another device: no remote copies, remote signals or barrier semaphores. Data moves between devices by JAX's collectives and lax.ppermute only.
A program may use at most 64 MiB of HBM per device.

```python
import math
import jax
import jax.numpy as jnp
from jax import lax

D = 256
HEADS = 4
HEAD_DIM = 64
BLK = 128
MAXB = 16
U_DEV = 4
CAND = 64
ITEM_DEV = 4096
TH = 256
USERS = 512
ITEMS = 524288
CAP = 4
DEVICES = 128


def pick_candidates(key):
    impressions = U_DEV * CAND
    slot_total = DEVICES * CAP

    def per_device(device_key):
        key_order, key_full, key_shuffle, key_row = jax.random.split(device_key, 4)
        visit = jax.random.permutation(key_order, slot_total)
        ranking = jnp.zeros((slot_total,), jnp.int32).at[visit].set(jnp.arange(slot_total, dtype=jnp.int32))
        full_owner = jax.random.randint(key_full, (), 0, DEVICES)
        slot_owner = jnp.arange(slot_total, dtype=jnp.int32) // CAP
        priority = ranking - jnp.where(slot_owner == full_owner, slot_total, 0)
        chosen = jnp.argsort(priority)[:impressions].astype(jnp.int32)
        chosen = jax.random.permutation(key_shuffle, chosen)
        owner_device = chosen // CAP
        item_row = jax.random.randint(key_row, (impressions,), 0, ITEM_DEV)
        return (owner_device * ITEM_DEV + item_row).astype(jnp.int32)
    return jax.vmap(per_device)(jax.random.split(key, DEVICES)).reshape(USERS, CAND)


def make_table(key):
    return jax.random.truncated_normal(key, -6.0, 6.0, (ITEMS, 2 * D), jnp.float32)


def draw_candidates(key, part):
    return pick_candidates(jax.random.fold_in(key, 11))


def draw_item_table(key, part):
    return make_table(jax.random.fold_in(key, 12)).astype(jnp.bfloat16)


def draw_lengths(key, part):
    level_key, length_key = jax.random.split(jax.random.fold_in(key, 21))
    levels = jax.random.randint(level_key, (DEVICES, 1), 0, 4)
    highest = jnp.maximum(jnp.right_shift(jnp.full((DEVICES, 1), MAXB * BLK, jnp.int32), levels), BLK // 8 + 1)
    drawn = jax.random.randint(length_key, (DEVICES, U_DEV), BLK // 8, highest + 1)
    drawn = drawn.at[0, 0].set(MAXB * BLK).at[0, 1].set(BLK // 8)
    return drawn.reshape(USERS).astype(jnp.int32)


def draw_history(key, part):
    base_key = jax.random.fold_in(key, 13)
    return jax.random.truncated_normal(base_key, -6.0, 6.0, (USERS, MAXB * BLK, D), jnp.float32).astype(jnp.bfloat16)


def gaussian(own_key, extent, deviation, most, kind=jnp.bfloat16):
    values = jax.random.normal(own_key, extent, jnp.float32) * deviation
    return jnp.minimum(jnp.maximum(values, -most), most).astype(kind)


def setup_inputs(seed: int = 0) -> dict:
    seeds = jax.random.split(jax.random.key(seed), 10)
    return {
        "history": draw_history(jax.random.fold_in(seeds[9], 71), 0),
        "lengths": draw_lengths(jax.random.fold_in(seeds[9], 71), 0),
        "candidates": draw_candidates(jax.random.fold_in(seeds[9], 71), 0),
        "item_table": draw_item_table(jax.random.fold_in(seeds[9], 71), 0),
        "value_weight": gaussian(seeds[4], (D, D), D ** -0.5, 0.375),
        "click_hidden": gaussian(seeds[5], (3 * D, TH), (3 * D) ** -0.5, 0.21875),
        "convert_hidden": gaussian(seeds[6], (3 * D, TH), (3 * D) ** -0.5, 0.21875),
        "click_output": gaussian(seeds[7], (TH,), (TH // 4) ** -0.5, 0.75),
        "convert_output": gaussian(seeds[8], (TH,), (TH // 4) ** -0.5, 0.75),
    }


def reference(history, lengths, candidates, item_table, value_weight, click_hidden, convert_hidden, click_output, convert_output):
    scale_factor = 1.0 / math.sqrt(HEAD_DIM)
    candidate_rows = item_table[candidates]
    target = candidate_rows[:, :, :D]
    features = candidate_rows[:, :, D:]
    value_heads = value_weight.astype(jnp.float32).reshape(D, HEADS, HEAD_DIM)

    def one_user(user_args):
        user_history, user_length, user_target = user_args
        blocks = user_history.reshape(MAXB, BLK, D).astype(jnp.float32)
        block_heads = blocks.reshape(MAXB, BLK, HEADS, HEAD_DIM)
        query = user_target.astype(jnp.float32).reshape(CAND, HEADS, HEAD_DIM)
        scores = jnp.einsum('chj,bthj->bcht', query, block_heads) * scale_factor
        place = jnp.arange(MAXB, dtype=jnp.int32)[:, None] * BLK + jnp.arange(BLK, dtype=jnp.int32)[None, :]
        live_key = (place < user_length)[:, None, None, :]
        masked = jnp.where(live_key, scores, -1e+30)
        block_max = lax.optimization_barrier(jnp.max(masked, -1))
        weights = jnp.where(live_key, jnp.exp(masked - block_max[..., None]), 0.0).astype(jnp.bfloat16)
        block_sum = lax.optimization_barrier(jnp.sum(weights.astype(jnp.float32), -1))
        block_context = jnp.einsum('bcht,btd->bchd', weights.astype(jnp.float32), blocks)
        top_max = lax.optimization_barrier(jnp.max(block_max, 0))
        factor = jnp.exp(block_max - top_max)
        total = lax.optimization_barrier(jnp.sum(factor * block_sum, 0))
        context = lax.optimization_barrier(jnp.sum(factor[..., None] * block_context, 0))
        numerator = jnp.einsum('chd,dhk->chk', context, value_heads, precision=lax.Precision.HIGHEST)
        pooled = (numerator / total[..., None]).reshape(CAND, D)
        normed = pooled * lax.rsqrt(lax.optimization_barrier(jnp.mean(pooled * pooled, -1, keepdims=True)) + 1e-06)
        return normed.astype(jnp.bfloat16)
    interest = lax.map(one_user, (history, lengths, target))
    joined = jnp.concatenate([interest, target, features], -1).reshape(USERS * CAND, 3 * D)
    click_act = jax.nn.relu(jnp.dot(joined, click_hidden, preferred_element_type=jnp.float32)).astype(jnp.bfloat16)
    convert_act = jax.nn.relu(jnp.dot(joined, convert_hidden, preferred_element_type=jnp.float32)).astype(jnp.bfloat16)
    click_rate = jax.nn.sigmoid(jnp.dot(click_act, click_output, preferred_element_type=jnp.float32))
    convert_rate = jax.nn.sigmoid(jnp.dot(convert_act, convert_output, preferred_element_type=jnp.float32))
    return (click_rate.reshape(USERS, CAND), (click_rate * convert_rate).reshape(USERS, CAND))
```

```python
import functools
import math

import jax
import jax.numpy as jnp
from jax import lax
from jax.experimental import pallas as pl
from jax.experimental.pallas import tpu as pltpu
from jax.sharding import PartitionSpec as P

HEADS = 4
SLOTS = 4
LANES = 128
CHUNK = 512
AXES = ("gx", "gy")
NEG = -1e30

F32 = jnp.float32
BF16 = jnp.bfloat16


def iota(shape, dim):
    return lax.broadcasted_iota(jnp.int32, shape, dim)


def ones_where(cond):
    return jnp.where(cond, 1.0, 0.0).astype(BF16)


def mm(a, b):
    return lax.dot_general(a, b, (((1,), (0,)), ((), ())), preferred_element_type=F32)


def mm_nt(a, b):
    return lax.dot_general(a, b, (((1,), (1,)), ((), ())), preferred_element_type=F32)


def request_kernel(cand_ref, req_ref, slot_ref, *, owners, row_bits):
    users, cands = cand_ref.shape
    total = users * cands
    ids = jnp.concatenate([cand_ref[u : u + 1, :] for u in range(users)], axis=1)
    owner = lax.shift_right_logical(ids, row_bits)
    row = jnp.bitwise_and(ids, (1 << row_bits) - 1)
    high = lax.shift_right_logical(row, 8).astype(F32)
    low = jnp.bitwise_and(row, 255).astype(F32)
    match = iota((owners, total), 0) == owner
    before = ones_where(iota((total, total), 0) < iota((total, total), 1))
    rank = mm(ones_where(match), before)
    place = jnp.sum(jnp.where(match, rank, 0.0), axis=0, keepdims=True) + (owner * SLOTS).astype(F32)
    slot_ref[...] = jnp.broadcast_to(place, slot_ref.shape)
    lane = iota((LANES, total), 0)
    picks, values = [], []
    for s in range(SLOTS):
        picks.append(ones_where(match & (rank == float(s))))
        values.append(
            jnp.where(lane == 2 * s, high, jnp.where(lane == 2 * s + 1, low, 0.0)).astype(BF16)
        )
    req_ref[...] = mm_nt(jnp.concatenate(picks, axis=1), jnp.concatenate(values, axis=1))


def answer_kernel(req_ref, table_ref, out_ref, hot_ref, high_ref, acc_ref, *, step):
    sources = req_ref.shape[0]
    rows = sources * SLOTS
    width = table_ref.shape[1]
    spread = ones_where(lax.shift_right_logical(iota((rows, sources), 0), 2) == iota((rows, sources), 1))
    asked = mm(spread, req_ref[...].astype(BF16))
    own = lax.shift_right_logical(iota((rows, LANES), 1), 1) == jnp.bitwise_and(iota((rows, LANES), 0), 3)
    asked = jnp.where(own, asked, 0.0).astype(BF16)
    which = jnp.bitwise_and(iota((LANES, 512), 0), 1) == lax.shift_right_logical(iota((LANES, 512), 1), 8)
    both = mm(asked, ones_where(which))
    high_ref[...] = both[:, :256].astype(BF16)
    hot_ref[...] = ones_where(both[:, 256:] == iota((rows, 256), 1).astype(F32))
    tiles = step // 256

    def body(t, carry):
        parts = []
        for k in range(tiles):
            index = jnp.full((1, 256), t * tiles + k, jnp.int32).astype(F32).astype(BF16)
            parts.append(jnp.where(high_ref[...] == index, hot_ref[...], jnp.zeros((), BF16)))
        part = mm(jnp.concatenate(parts, axis=1), table_ref[pl.ds(t * step, step), :])

        @pl.when(t == 0)
        def _():
            acc_ref[...] = part

        @pl.when(t > 0)
        def _():
            acc_ref[...] += part

        return carry

    lax.fori_loop(0, table_ref.shape[0] // step, body, 0)
    quarter = [
        acc_ref[:, q * LANES : (q + 1) * LANES].reshape(rows // 8, 8, LANES) for q in range(width // LANES)
    ]
    first = iota((rows // 8, 8, LANES), 1) < 4

    def even(a, b):
        return jnp.where(first, a, pltpu.roll(b, 4, axis=1))

    def odd(a, b):
        return jnp.where(first, pltpu.roll(a, 4, axis=1), b)

    packed = jnp.concatenate(
        [
            even(quarter[0], quarter[1]),
            even(quarter[2], quarter[3]),
            odd(quarter[0], quarter[1]),
            odd(quarter[2], quarter[3]),
        ],
        axis=1,
    )
    out_ref[...] = packed.reshape(rows * 4, LANES).astype(BF16)


def attend_kernel(
    len_ref,
    slot_ref,
    answer_ref,
    history_ref,
    value_ref,
    click_ref,
    convert_ref,
    click_out_ref,
    convert_out_ref,
    rate_ref,
    both_ref,
    hist_ref,
    query_ref,
    joined_ref,
    acc_ref,
    max_ref,
    sum_ref,
    sem_ref,
):
    users, seq, width = hist_ref.shape
    cands = rate_ref.shape[1]
    head_width = width // HEADS
    total = users * cands
    pieces = seq // CHUNK
    rows = HEADS * cands

    def copy(u, j):
        part = pl.ds(j * CHUNK, CHUNK)
        return pltpu.make_async_copy(
            history_ref.at[u, part], hist_ref.at[u, part], sem_ref.at[u, j]
        )

    for u in range(users):
        for j in range(pieces):

            @pl.when(len_ref[u] > j * CHUNK)
            def _():
                copy(u, j).start()

    group = answer_ref.shape[0] // 32
    got = answer_ref[...].astype(F32).reshape(group, 32, LANES)
    a0, b0, a1, b1 = (got[:, 8 * k : 8 * k + 8] for k in range(4))
    first = iota((group, 8, LANES), 1) < 4
    quarters = [
        jnp.where(first, a0, pltpu.roll(a1, 4, axis=1)),
        jnp.where(first, pltpu.roll(a0, 4, axis=1), a1),
        jnp.where(first, b0, pltpu.roll(b1, 4, axis=1)),
        jnp.where(first, pltpu.roll(b0, 4, axis=1), b1),
    ]
    answers = jnp.concatenate([q.reshape(group * 8, LANES).astype(BF16) for q in quarters], axis=1)
    place = jnp.transpose(slot_ref[...])[:, 0:1]
    pick = ones_where(place == iota((total, group * 8), 1).astype(F32))
    rows_got = mm(pick, answers)
    joined_ref[:, width:] = rows_got.astype(BF16)
    head_of_lane = lax.shift_right_logical(iota((cands, width), 1), head_width.bit_length() - 1)
    for u in range(users):
        target = rows_got[u * cands : (u + 1) * cands, :width] * (1.0 / math.sqrt(head_width))
        for h in range(HEADS):
            query_ref[u, h * cands : (h + 1) * cands, :] = jnp.where(
                head_of_lane == h, target, 0.0
            ).astype(BF16)

    acc_ref[...] = jnp.zeros(acc_ref.shape, F32)
    sum_ref[...] = jnp.zeros(sum_ref.shape, F32)
    max_ref[...] = jnp.full(max_ref.shape, NEG, F32)
    lane = iota((1, CHUNK), 1)
    for u in range(users):

        def body(j, carry):
            copy(u, j).wait()
            block = hist_ref[u, pl.ds(j * CHUNK, CHUNK), :]
            scores = mm_nt(query_ref[u], block)
            scores = jnp.where(lane < len_ref[u] - j * CHUNK, scores, NEG)
            old = max_ref[u]
            new = jnp.maximum(old, jnp.max(scores, axis=1, keepdims=True))
            scale = jnp.exp(old - new)
            added = sum_ref[u] * scale
            weights = []
            for k in range(CHUNK // LANES):
                w = jnp.exp(scores[:, k * LANES : (k + 1) * LANES] - new).astype(BF16)
                added += w.astype(F32)
                weights.append(w)
            max_ref[u] = new
            sum_ref[u] = added
            context = mm(jnp.concatenate(weights, axis=1), block)
            for k in range(width // LANES):
                part = slice(k * LANES, (k + 1) * LANES)
                acc_ref[u, :, part] = acc_ref[u, :, part] * scale + context[:, part]
            return carry

        lax.fori_loop(0, (len_ref[u] + CHUNK - 1) // CHUNK, body, 0)

    for u in range(users):
        context = acc_ref[u]
        coarse = context.astype(BF16)
        fine = (context - coarse.astype(F32)).astype(BF16)
        number = mm(coarse, value_ref[...]) + mm(fine, value_ref[...])
        number = number / jnp.sum(sum_ref[u], axis=1, keepdims=True)
        pooled = jnp.zeros((cands, width), F32)
        for h in range(HEADS):
            pooled = jnp.where(head_of_lane == h, number[h * cands : (h + 1) * cands], pooled)
        square = jnp.mean(pooled * pooled, axis=1, keepdims=True)
        joined_ref[u * cands : (u + 1) * cands, :width] = (pooled * lax.rsqrt(square + 1e-06)).astype(BF16)

    joined = joined_ref[...]

    def tower(hidden_ref, out_ref):
        act = jnp.maximum(mm(joined, hidden_ref[...]), 0.0).astype(BF16)
        logit = mm_nt(jnp.broadcast_to(out_ref[...], (16, out_ref.shape[1])), act)
        return jax.nn.sigmoid(logit[0:1])

    rate = tower(click_ref, click_out_ref)
    both = rate * tower(convert_ref, convert_out_ref)
    for u in range(users):
        rate_ref[u : u + 1, :] = rate[:, u * cands : (u + 1) * cands]
        both_ref[u : u + 1, :] = both[:, u * cands : (u + 1) * cands]


def vmem():
    return pl.BlockSpec(memory_space=pltpu.VMEM)


def local(
    history,
    lengths,
    candidates,
    item_table,
    value_weight,
    click_hidden,
    convert_hidden,
    click_output,
    convert_output,
):
    users, seq, width = history.shape
    cands = candidates.shape[1]
    table_rows, row_width = item_table.shape
    devices = lax.axis_size("gx") * lax.axis_size("gy")
    total = users * cands
    params = pltpu.CompilerParams(vmem_limit_bytes=40 << 20)

    request, place = pl.pallas_call(
        functools.partial(request_kernel, owners=devices, row_bits=table_rows.bit_length() - 1),
        out_shape=(
            jax.ShapeDtypeStruct((devices, LANES), F32),
            jax.ShapeDtypeStruct((8, total), F32),
        ),
        in_specs=[vmem()],
        out_specs=(vmem(), vmem()),
        name="request",
    )(candidates)
    asked = lax.all_to_all(request, AXES, 0, 0, tiled=True)
    answer = pl.pallas_call(
        functools.partial(answer_kernel, step=512),
        out_shape=jax.ShapeDtypeStruct((devices * 16, LANES), BF16),
        in_specs=[vmem(), vmem()],
        out_specs=vmem(),
        scratch_shapes=[
            pltpu.VMEM((devices * SLOTS, 256), BF16),
            pltpu.VMEM((devices * SLOTS, 256), BF16),
            pltpu.VMEM((devices * SLOTS, row_width), F32),
        ],
        compiler_params=params,
        name="answer",
    )(asked, item_table)
    answered = lax.all_to_all(answer, AXES, 0, 0, tiled=True)
    return pl.pallas_call(
        attend_kernel,
        out_shape=(
            jax.ShapeDtypeStruct((users, cands), F32),
            jax.ShapeDtypeStruct((users, cands), F32),
        ),
        in_specs=[
            pl.BlockSpec(memory_space=pltpu.SMEM),
            vmem(),
            vmem(),
            pl.BlockSpec(memory_space=pl.ANY),
            vmem(),
            vmem(),
            vmem(),
            vmem(),
            vmem(),
        ],
        out_specs=(vmem(), vmem()),
        scratch_shapes=[
            pltpu.VMEM((users, seq, width), BF16),
            pltpu.VMEM((users, HEADS * cands, width), BF16),
            pltpu.VMEM((total, 3 * width), BF16),
            pltpu.VMEM((users, HEADS * cands, width), F32),
            pltpu.VMEM((users, HEADS * cands, LANES), F32),
            pltpu.VMEM((users, HEADS * cands, LANES), F32),
            pltpu.SemaphoreType.DMA((users, seq // CHUNK)),
        ],
        compiler_params=params,
        name="attend",
    )(
        lengths,
        place,
        answered,
        history,
        value_weight,
        click_hidden,
        convert_hidden,
        click_output.reshape(1, -1),
        convert_output.reshape(1, -1),
    )


def solution(mesh):
    split = P(AXES)
    return jax.shard_map(
        local,
        mesh=mesh,
        in_specs=(split, split, split, split, P(), P(), P(), P(), P()),
        out_specs=(split, split),
        check_vma=False,
    )
```

```python
import functools
import math

import jax
import jax.numpy as jnp
from jax import lax
from jax.experimental import pallas as pl
from jax.experimental.pallas import tpu as pltpu
from jax.sharding import PartitionSpec as P

HEADS = 4
SLOTS = 4
LANES = 128
CHUNK = 512
AXES = ("gx", "gy")
NEG = -1e30

F32 = jnp.float32
BF16 = jnp.bfloat16


def iota(shape, dim):
    return lax.broadcasted_iota(jnp.int32, shape, dim)


def ones_where(cond):
    return jnp.where(cond, 1.0, 0.0).astype(BF16)


def mm(a, b):
    return lax.dot_general(a, b, (((1,), (0,)), ((), ())), preferred_element_type=F32)


def mm_nt(a, b):
    return lax.dot_general(a, b, (((1,), (1,)), ((), ())), preferred_element_type=F32)


def request_kernel(cand_ref, req_ref, slot_ref, *, owners, row_bits):
    users, cands = cand_ref.shape
    total = users * cands
    ids = jnp.concatenate([cand_ref[u : u + 1, :] for u in range(users)], axis=1)
    owner = lax.shift_right_logical(ids, row_bits)
    row = jnp.bitwise_and(ids, (1 << row_bits) - 1)
    high = lax.shift_right_logical(row, 8).astype(F32)
    low = jnp.bitwise_and(row, 255).astype(F32)
    match = iota((owners, total), 0) == owner
    before = ones_where(iota((total, total), 0) < iota((total, total), 1))
    rank = mm(ones_where(match), before)
    place = jnp.sum(jnp.where(match, rank, 0.0), axis=0, keepdims=True) + (owner * SLOTS).astype(F32)
    slot_ref[...] = jnp.broadcast_to(place, slot_ref.shape)
    lane = iota((LANES, total), 0)
    picks, values = [], []
    for s in range(SLOTS):
        picks.append(ones_where(match & (rank == float(s))))
        values.append(
            jnp.where(lane == 2 * s, high, jnp.where(lane == 2 * s + 1, low, 0.0)).astype(BF16)
        )
    req_ref[...] = mm_nt(jnp.concatenate(picks, axis=1), jnp.concatenate(values, axis=1))


def answer_kernel(req_ref, staged_ref, table_ref, out_ref, hot_ref, high_ref, acc_ref, rest_ref, sem_ref):
    sources = req_ref.shape[0]
    rows = sources * SLOTS
    staged, width = staged_ref.shape
    rest = pltpu.make_async_copy(table_ref.at[pl.ds(staged, rest_ref.shape[0])], rest_ref, sem_ref)
    rest.start()
    spread = ones_where(lax.shift_right_logical(iota((rows, sources), 0), 2) == iota((rows, sources), 1))
    asked = mm(spread, req_ref[...].astype(BF16))
    own = lax.shift_right_logical(iota((rows, LANES), 1), 1) == jnp.bitwise_and(iota((rows, LANES), 0), 3)
    asked = jnp.where(own, asked, 0.0).astype(BF16)
    which = jnp.bitwise_and(iota((LANES, 512), 0), 1) == lax.shift_right_logical(iota((LANES, 512), 1), 8)
    both = mm(asked, ones_where(which))
    high_ref[...] = both[:, :256].astype(BF16)
    hot_ref[...] = ones_where(both[:, 256:] == iota((rows, 256), 1).astype(F32))

    def part(first, part_ref):
        hot = [
            jnp.where(high_ref[...] == jnp.array(first + k, BF16), hot_ref[...], jnp.zeros((), BF16))
            for k in range(part_ref.shape[0] // 256)
        ]
        return mm(jnp.concatenate(hot, axis=1), part_ref[...])

    acc_ref[...] = part(0, staged_ref)
    rest.wait()
    acc_ref[...] += part(staged // 256, rest_ref)
    quarter = [
        acc_ref[:, q * LANES : (q + 1) * LANES].reshape(rows // 8, 8, LANES) for q in range(width // LANES)
    ]
    first = iota((rows // 8, 8, LANES), 1) < 4

    def even(a, b):
        return jnp.where(first, a, pltpu.roll(b, 4, axis=1))

    def odd(a, b):
        return jnp.where(first, pltpu.roll(a, 4, axis=1), b)

    packed = jnp.concatenate(
        [
            even(quarter[0], quarter[1]),
            even(quarter[2], quarter[3]),
            odd(quarter[0], quarter[1]),
            odd(quarter[2], quarter[3]),
        ],
        axis=1,
    )
    out_ref[...] = packed.reshape(rows * 4, LANES).astype(BF16)


def attend_kernel(
    len_ref,
    slot_ref,
    answer_ref,
    history_ref,
    value_hbm_ref,
    click_hbm_ref,
    convert_hbm_ref,
    click_out_ref,
    convert_out_ref,
    rate_ref,
    both_ref,
    hist_ref,
    value_ref,
    click_ref,
    convert_ref,
    query_ref,
    joined_ref,
    acc_ref,
    max_ref,
    sum_ref,
    score_a_ref,
    score_b_ref,
    item_ref,
    hist_sem,
    weight_sem,
):
    users, seq, width = history_ref.shape
    cands = rate_ref.shape[1]
    head_width = width // HEADS
    total = users * cands
    pieces = seq // CHUNK

    def copy(u, j):
        part = pl.ds(j * CHUNK, CHUNK)
        return pltpu.make_async_copy(history_ref.at[u, part], hist_ref.at[u, part], hist_sem.at[u, j])

    weights = [
        pltpu.make_async_copy(source, target, weight_sem.at[k])
        for k, (source, target) in enumerate(
            ((value_hbm_ref, value_ref), (click_hbm_ref, click_ref), (convert_hbm_ref, convert_ref))
        )
    ]

    items = jnp.int32(0)
    for u in range(users):
        for j in range(pieces):

            @pl.when(len_ref[u] > j * CHUNK)
            def _():
                item_ref[items + j] = u * pieces + j
                copy(u, j).start()

        items += lax.div(len_ref[u] + (CHUNK - 1), CHUNK)
    for weight in weights:
        weight.start()

    group = answer_ref.shape[0] // 32
    got = answer_ref[...].astype(F32).reshape(group, 32, LANES)
    a0, b0, a1, b1 = (got[:, 8 * k : 8 * k + 8] for k in range(4))
    first = iota((group, 8, LANES), 1) < 4
    quarters = [
        jnp.where(first, a0, pltpu.roll(a1, 4, axis=1)),
        jnp.where(first, pltpu.roll(a0, 4, axis=1), a1),
        jnp.where(first, b0, pltpu.roll(b1, 4, axis=1)),
        jnp.where(first, pltpu.roll(b0, 4, axis=1), b1),
    ]
    answers = jnp.concatenate([q.reshape(group * 8, LANES).astype(BF16) for q in quarters], axis=1)
    place = jnp.transpose(slot_ref[...])[:, 0:1]
    pick = ones_where(place == iota((total, group * 8), 1).astype(F32))
    rows_got = mm(pick, answers)
    joined_ref[:, width:] = rows_got.astype(BF16)
    head_of_lane = lax.shift_right_logical(iota((cands, width), 1), head_width.bit_length() - 1)
    for u in range(users):
        target = rows_got[u * cands : (u + 1) * cands, :width] * (1.0 / math.sqrt(head_width))
        for h in range(HEADS):
            query_ref[u, h * cands : (h + 1) * cands, :] = jnp.where(
                head_of_lane == h, target, 0.0
            ).astype(BF16)

    acc_ref[...] = jnp.zeros(acc_ref.shape, F32)
    sum_ref[...] = jnp.zeros(sum_ref.shape, F32)
    max_ref[...] = jnp.full(max_ref.shape, NEG, F32)
    lane = iota((1, CHUNK), 1)

    def user_and_piece(i):
        item = item_ref[i]
        return lax.div(item, pieces), lax.rem(item, pieces)

    def arrive(i):
        @pl.when(i < items)
        def _():
            copy(*user_and_piece(i)).wait()

    def score(i, score_ref):
        u, j = user_and_piece(jnp.minimum(i, items - 1))
        scores = mm_nt(query_ref[u], hist_ref[u, pl.ds(j * CHUNK, CHUNK), :])
        scores = jnp.where(lane < len_ref[u] - j * CHUNK, scores, NEG)
        score_ref[...] = scores

    def gather(i, score_ref):
        u, j = user_and_piece(i)
        block = hist_ref[u, pl.ds(j * CHUNK, CHUNK), :]
        old = max_ref[u]
        new = jnp.maximum(old, jnp.max(score_ref[...], axis=1, keepdims=True))
        scale = jnp.exp(old - new)
        max_ref[u] = new
        added = sum_ref[u] * scale
        weight = []
        for k in range(CHUNK // LANES):
            w = jnp.exp(score_ref[:, k * LANES : (k + 1) * LANES] - new)
            added += w
            weight.append(w.astype(BF16))
        sum_ref[u] = added
        context = mm(jnp.concatenate(weight, axis=1), block)
        for k in range(width // LANES):
            part = slice(k * LANES, (k + 1) * LANES)
            acc_ref[u, :, part] = acc_ref[u, :, part] * scale + context[:, part]

    arrive(0)
    score(0, score_a_ref)

    def pair(p, carry):
        i = 2 * p
        arrive(i + 1)
        score(i + 1, score_b_ref)
        gather(i, score_a_ref)
        arrive(i + 2)

        @pl.when(i + 1 < items)
        def _():
            score(i + 2, score_a_ref)
            gather(i + 1, score_b_ref)

        return carry

    lax.fori_loop(0, lax.div(items + 1, 2), pair, 0)
    for weight in weights:
        weight.wait()

    row = iota((LANES, 1), 0)
    nothing = jnp.zeros((LANES, width), F32)
    click_out = jnp.where(row == 0, click_out_ref[...].astype(F32), nothing)
    convert_out = jnp.where(row == 1, convert_out_ref[...].astype(F32), nothing)
    out_weight = jnp.concatenate([click_out, convert_out], axis=1).astype(BF16)
    towers = (click_ref, convert_ref)
    early = [mm(joined_ref[:, width:], hidden[width:, :]) for hidden in towers]

    context = acc_ref[...].reshape(users * HEADS * cands, width)
    coarse = context.astype(BF16)
    fine = (context - coarse.astype(F32)).astype(BF16)
    number = mm(coarse, value_ref[...]) + mm(fine, value_ref[...])
    interest = []
    for u in range(users):
        above = jnp.zeros((cands, width), F32)
        below = jnp.ones((cands, width), F32)
        for h in range(HEADS):
            head = slice(h * cands, (h + 1) * cands)
            above = jnp.where(head_of_lane == h, number[u * HEADS * cands :][head], above)
            below = jnp.where(head_of_lane == h, jnp.sum(sum_ref[u, head], axis=1, keepdims=True), below)
        pooled = above / below
        square = jnp.mean(pooled * pooled, axis=1, keepdims=True)
        interest.append((pooled * lax.rsqrt(square + 1e-06)).astype(BF16))
    interest = jnp.concatenate(interest, axis=0)
    act = jnp.concatenate(
        [
            jnp.maximum(mm(interest, hidden[:width, :]) + part, 0.0).astype(BF16)
            for hidden, part in zip(towers, early)
        ],
        axis=1,
    )
    logit = jnp.transpose(mm_nt(act, out_weight))
    rate = jax.nn.sigmoid(logit[0:1])
    both = rate * jax.nn.sigmoid(logit[1:2])
    for u in range(users):
        rate_ref[u : u + 1, :] = rate[:, u * cands : (u + 1) * cands]
        both_ref[u : u + 1, :] = both[:, u * cands : (u + 1) * cands]


def stage_kernel(from_ref, to_ref, sem_ref):
    copy = pltpu.make_async_copy(from_ref.at[pl.ds(0, to_ref.shape[0])], to_ref, sem_ref)
    copy.start()
    copy.wait()


def stage(x, count):
    staged = pl.pallas_call(
        stage_kernel,
        out_shape=pltpu.VMEM((count,) + x.shape[1:], x.dtype),
        in_specs=[hbm()],
        out_specs=vmem(),
        scratch_shapes=[pltpu.SemaphoreType.DMA(())],
        cost_estimate=pl.CostEstimate(flops=1 << 30, bytes_accessed=2 * x.size, transcendentals=0),
        compiler_params=limit(2),
        name="stage",
    )(x)
    return pltpu.with_memory_space_constraint(staged, pltpu.VMEM)


def hbm():
    return pl.BlockSpec(memory_space=pltpu.HBM)


def limit(mib):
    return pltpu.CompilerParams(vmem_limit_bytes=mib << 20)


def vmem():
    return pl.BlockSpec(memory_space=pltpu.VMEM)


def local(
    history,
    lengths,
    candidates,
    item_table,
    value_weight,
    click_hidden,
    convert_hidden,
    click_output,
    convert_output,
):
    users, seq, width = history.shape
    cands = candidates.shape[1]
    table_rows, row_width = item_table.shape
    devices = lax.axis_size("gx") * lax.axis_size("gy")
    total = users * cands
    rows = HEADS * cands
    table = pltpu.with_memory_space_constraint(item_table, pltpu.HBM)
    staged = 5 * table_rows // 8

    request, place = pl.pallas_call(
        functools.partial(request_kernel, owners=devices, row_bits=table_rows.bit_length() - 1),
        out_shape=(pltpu.VMEM((devices, LANES), F32), pltpu.VMEM((8, total), F32)),
        in_specs=[vmem()],
        out_specs=(vmem(), vmem()),
        compiler_params=limit(8),
        name="request",
    )(candidates)
    asked = lax.all_to_all(request, AXES, 0, 0, tiled=True)
    answer = pl.pallas_call(
        answer_kernel,
        out_shape=jax.ShapeDtypeStruct((devices * 16, LANES), BF16),
        in_specs=[vmem(), vmem(), hbm()],
        out_specs=vmem(),
        scratch_shapes=[
            pltpu.VMEM((devices * SLOTS, 256), BF16),
            pltpu.VMEM((devices * SLOTS, 256), BF16),
            pltpu.VMEM((devices * SLOTS, row_width), F32),
            pltpu.VMEM((table_rows - staged, row_width), BF16),
            pltpu.SemaphoreType.DMA(()),
        ],
        compiler_params=limit(24),
        name="answer",
    )(asked, stage(table, staged), table)
    answered = lax.all_to_all(answer, AXES, 0, 0, tiled=True)
    return pl.pallas_call(
        attend_kernel,
        out_shape=(
            jax.ShapeDtypeStruct((users, cands), F32),
            jax.ShapeDtypeStruct((users, cands), F32),
        ),
        in_specs=[pl.BlockSpec(memory_space=pltpu.SMEM), vmem(), vmem(), hbm(), hbm(), hbm(), hbm(), vmem(), vmem()],
        out_specs=(vmem(), vmem()),
        scratch_shapes=[
            pltpu.VMEM((users, seq, width), BF16),
            pltpu.VMEM(value_weight.shape, BF16),
            pltpu.VMEM(click_hidden.shape, BF16),
            pltpu.VMEM(convert_hidden.shape, BF16),
            pltpu.VMEM((users, rows, width), BF16),
            pltpu.VMEM((total, 3 * width), BF16),
            pltpu.VMEM((users, rows, width), F32),
            pltpu.VMEM((users, rows, LANES), F32),
            pltpu.VMEM((users, rows, LANES), F32),
            pltpu.VMEM((rows, CHUNK), F32),
            pltpu.VMEM((rows, CHUNK), F32),
            pltpu.SMEM((users * (seq // CHUNK) + 1,), jnp.int32),
            pltpu.SemaphoreType.DMA((users, seq // CHUNK)),
            pltpu.SemaphoreType.DMA((3,)),
        ],
        compiler_params=limit(24),
        name="attend",
    )(
        lengths,
        place,
        answered,
        *(
            pltpu.with_memory_space_constraint(x, pltpu.HBM)
            for x in (history, value_weight, click_hidden, convert_hidden)
        ),
        click_output.reshape(1, -1),
        convert_output.reshape(1, -1),
    )


def solution(mesh):
    split = P(AXES)
    return jax.shard_map(
        local,
        mesh=mesh,
        in_specs=(split, split, split, split, P(), P(), P(), P(), P()),
        out_specs=(split, split),
        check_vma=False,
    )
```

```python
import functools
import math

import jax
import jax.numpy as jnp
from jax import lax
from jax.experimental import pallas as pl
from jax.experimental.pallas import tpu as pltpu
from jax.sharding import PartitionSpec as P

HEADS = 4
SLOTS = 4
LANES = 128
CHUNK = 512
AXES = ("gx", "gy")
NEG = -1e30

F32 = jnp.float32
BF16 = jnp.bfloat16


def iota(shape, dim):
    return lax.broadcasted_iota(jnp.int32, shape, dim)


def ones_where(cond):
    return jnp.where(cond, 1.0, 0.0).astype(BF16)


def mm(a, b):
    return lax.dot_general(a, b, (((1,), (0,)), ((), ())), preferred_element_type=F32)


def mm_nt(a, b):
    return lax.dot_general(a, b, (((1,), (1,)), ((), ())), preferred_element_type=F32)


def request_kernel(cand_ref, req_ref, slot_ref, *, owners, row_bits):
    users, cands = cand_ref.shape
    total = users * cands
    ids = jnp.concatenate([cand_ref[u : u + 1, :] for u in range(users)], axis=1)
    owner = lax.shift_right_logical(ids, row_bits)
    row = jnp.bitwise_and(ids, (1 << row_bits) - 1)
    high = lax.shift_right_logical(row, 8).astype(F32)
    low = jnp.bitwise_and(row, 255).astype(F32)
    match = iota((owners, total), 0) == owner
    before = ones_where(iota((total, total), 0) < iota((total, total), 1))
    rank = mm(ones_where(match), before)
    place = jnp.sum(jnp.where(match, rank, 0.0), axis=0, keepdims=True) + (owner * SLOTS).astype(F32)
    slot_ref[...] = jnp.broadcast_to(place, slot_ref.shape)
    lane = iota((LANES, total), 0)
    picks, values = [], []
    for s in range(SLOTS):
        picks.append(ones_where(match & (rank == float(s))))
        values.append(
            jnp.where(lane == 2 * s, high, jnp.where(lane == 2 * s + 1, low, 0.0)).astype(BF16)
        )
    req_ref[...] = mm_nt(jnp.concatenate(picks, axis=1), jnp.concatenate(values, axis=1))


def answer_kernel(req_ref, staged_ref, table_ref, out_ref, hot_ref, high_ref, acc_ref, rest_ref, sem_ref):
    sources = req_ref.shape[0]
    rows = sources * SLOTS
    staged, width = staged_ref.shape
    rest = pltpu.make_async_copy(table_ref.at[pl.ds(staged, rest_ref.shape[0])], rest_ref, sem_ref)
    rest.start()
    spread = ones_where(lax.shift_right_logical(iota((rows, sources), 0), 2) == iota((rows, sources), 1))
    asked = mm(spread, req_ref[...].astype(BF16))
    own = lax.shift_right_logical(iota((rows, LANES), 1), 1) == jnp.bitwise_and(iota((rows, LANES), 0), 3)
    asked = jnp.where(own, asked, 0.0).astype(BF16)
    which = jnp.bitwise_and(iota((LANES, 512), 0), 1) == lax.shift_right_logical(iota((LANES, 512), 1), 8)
    both = mm(asked, ones_where(which))
    high_ref[...] = both[:, :256].astype(BF16)
    hot_ref[...] = ones_where(both[:, 256:] == iota((rows, 256), 1).astype(F32))

    def part(first, part_ref):
        hot = [
            jnp.where(high_ref[...] == jnp.array(first + k, BF16), hot_ref[...], jnp.zeros((), BF16))
            for k in range(part_ref.shape[0] // 256)
        ]
        return mm(jnp.concatenate(hot, axis=1), part_ref[...])

    acc_ref[...] = part(0, staged_ref)
    rest.wait()
    acc_ref[...] += part(staged // 256, rest_ref)
    quarter = [
        acc_ref[:, q * LANES : (q + 1) * LANES].reshape(rows // 8, 8, LANES) for q in range(width // LANES)
    ]
    first = iota((rows // 8, 8, LANES), 1) < 4

    def even(a, b):
        return jnp.where(first, a, pltpu.roll(b, 4, axis=1))

    def odd(a, b):
        return jnp.where(first, pltpu.roll(a, 4, axis=1), b)

    packed = jnp.concatenate(
        [
            even(quarter[0], quarter[1]),
            even(quarter[2], quarter[3]),
            odd(quarter[0], quarter[1]),
            odd(quarter[2], quarter[3]),
        ],
        axis=1,
    )
    out_ref[...] = packed.reshape(rows * 4, LANES).astype(BF16)


def attend_kernel(
    len_hbm_ref,
    live_ref,
    pick_ref,
    answer_ref,
    last_ref,
    value_ref,
    click_ref,
    convert_ref,
    history_ref,
    click_out_ref,
    convert_out_ref,
    rate_ref,
    both_ref,
    hist_ref,
    query_ref,
    joined_ref,
    acc_ref,
    max_ref,
    sum_ref,
    score_a_ref,
    score_b_ref,
    weight_a_ref,
    weight_b_ref,
    scale_a_ref,
    scale_b_ref,
    early_ref,
    item_ref,
    len_ref,
    hist_sem,
    len_sem,
):
    users, seq, width = history_ref.shape
    cands = rate_ref.shape[1]
    head_width = width // HEADS
    total = users * cands
    pieces = seq // CHUNK

    def rest(u):
        part = pl.ds(0, seq - CHUNK)
        return pltpu.make_async_copy(history_ref.at[u, part], hist_ref.at[u], hist_sem.at[u])

    lengths = pltpu.make_async_copy(len_hbm_ref, len_ref, len_sem)
    lengths.start()

    group = answer_ref.shape[0] // 32
    got = answer_ref[...].astype(F32).reshape(group, 32, LANES)
    a0, b0, a1, b1 = (got[:, 8 * k : 8 * k + 8] for k in range(4))
    first = iota((group, 8, LANES), 1) < 4
    quarters = [
        jnp.where(first, a0, pltpu.roll(a1, 4, axis=1)),
        jnp.where(first, pltpu.roll(a0, 4, axis=1), a1),
        jnp.where(first, b0, pltpu.roll(b1, 4, axis=1)),
        jnp.where(first, pltpu.roll(b0, 4, axis=1), b1),
    ]
    answers = jnp.concatenate([q.reshape(group * 8, LANES).astype(BF16) for q in quarters], axis=1)
    rows_got = mm(pick_ref[...], answers)
    joined_ref[:, width:] = rows_got.astype(BF16)
    head_of_lane = lax.shift_right_logical(iota((cands, width), 1), head_width.bit_length() - 1)
    for u in range(users):
        target = rows_got[u * cands : (u + 1) * cands, :width] * (1.0 / math.sqrt(head_width))
        for h in range(HEADS):
            query_ref[u, h * cands : (h + 1) * cands, :] = jnp.where(
                head_of_lane == h, target, 0.0
            ).astype(BF16)

    lengths.wait()

    def begin(u, carry):
        @pl.when(len_ref[u] > CHUNK)
        def _():
            rest(u).start()

        return carry

    lax.fori_loop(0, users, begin, 0)

    towers = (click_ref, convert_ref)
    for k, hidden in enumerate(towers):
        early_ref[k] = mm(joined_ref[:, width:], hidden[width:, :])
    lane = iota((1, CHUNK), 1)

    def exp_parts(scores_of, top):
        added = None
        weight = []
        for k in range(CHUNK // LANES):
            w = jnp.exp(scores_of(slice(k * LANES, (k + 1) * LANES)) - top)
            added = w if added is None else added + w
            weight.append(w.astype(BF16))
        return jnp.concatenate(weight, axis=1), added

    for u in range(users):
        block = last_ref[u]
        live = jnp.concatenate([live_ref[u : u + 1, :]] * (CHUNK // LANES), axis=1)
        scores = jnp.where(lane < live, mm_nt(query_ref[u], block), NEG)
        top = jnp.broadcast_to(jnp.max(scores, axis=1, keepdims=True), (scores.shape[0], LANES))
        max_ref[u] = top
        weight, sum_ref[u] = exp_parts(lambda part: scores[:, part], top)
        acc_ref[u] = mm(weight, block)

    def enter(k, user, source, offset, wait):
        for field, value in enumerate((user, source, offset, wait)):
            item_ref[field, k] = value

    items = jnp.int32(0)
    for u in range(users):
        for j in range(1, pieces):

            @pl.when(len_ref[u] > j * CHUNK)
            def _():
                enter(items + (j + 1), u, u, (j - 1) * CHUNK, int(j == 1))

        items += lax.div(len_ref[u] - 1, CHUNK)
    for k in (0, 1, *(items + (k + 2) for k in range(5))):
        enter(k, users, 0, 0, 0)

    def entry(k):
        return tuple(item_ref[field, k] for field in range(4))

    def block(item):
        return hist_ref[item[1], pl.ds(pl.multiple_of(item[2], CHUNK), CHUNK), :]

    def step(now, ahead, beyond, score_to_ref, score_ref, weight_to_ref, scale_to_ref, weight_ref, scale_ref):
        score_to_ref[...] = mm_nt(query_ref[beyond[1]], block(beyond))

        u = ahead[0]
        old = max_ref[u]
        new = jnp.maximum(old, jnp.max(score_ref[...], axis=1, keepdims=True))
        scale = jnp.exp(old - new)
        max_ref[u] = new
        scale_to_ref[...] = scale
        weight_to_ref[...], added = exp_parts(lambda part: score_ref[:, part], new)
        sum_ref[u] = sum_ref[u] * scale + added

        u = now[0]
        context = mm(weight_ref[...], block(now))
        scale = scale_ref[...]
        for k in range(width // LANES):
            part = slice(k * LANES, (k + 1) * LANES)
            acc_ref[u, :, part] = acc_ref[u, :, part] * scale + context[:, part]

    def pair(p, carry):
        a, b, c, d = carry
        for item in (c, d):

            @pl.when(item[3] == 1)
            def _():
                rest(item[1]).wait()

        step(a, b, c, score_a_ref, score_b_ref, weight_b_ref, scale_b_ref, weight_a_ref, scale_a_ref)
        step(b, c, d, score_b_ref, score_a_ref, weight_a_ref, scale_a_ref, weight_b_ref, scale_b_ref)
        return c, d, entry(2 * p + 4), entry(2 * p + 5)

    @pl.when(items > 0)
    def _():
        lax.fori_loop(0, lax.div(items + 3, 2), pair, tuple(entry(k) for k in range(4)))

    row = iota((LANES, 1), 0)
    nothing = jnp.zeros((LANES, width), F32)
    click_out = jnp.where(row == 0, click_out_ref[...].astype(F32), nothing)
    convert_out = jnp.where(row == 1, convert_out_ref[...].astype(F32), nothing)
    out_weight = jnp.concatenate([click_out, convert_out], axis=1).astype(BF16)

    context = acc_ref[:users].reshape(users * HEADS * cands, width)
    number = mm(context.astype(BF16), value_ref[...])
    interest = []
    for u in range(users):
        above = jnp.zeros((cands, width), F32)
        below = jnp.ones((cands, width), F32)
        for h in range(HEADS):
            head = slice(h * cands, (h + 1) * cands)
            above = jnp.where(head_of_lane == h, number[u * HEADS * cands :][head], above)
            below = jnp.where(head_of_lane == h, jnp.sum(sum_ref[u, head], axis=1, keepdims=True), below)
        pooled = above / below
        square = jnp.mean(pooled * pooled, axis=1, keepdims=True)
        interest.append((pooled * lax.rsqrt(square + 1e-06)).astype(BF16))
    interest = jnp.concatenate(interest, axis=0)
    act = jnp.concatenate(
        [
            jnp.maximum(mm(interest, hidden[:width, :]) + early_ref[k], 0.0).astype(BF16)
            for k, hidden in enumerate(towers)
        ],
        axis=1,
    )
    logit = jnp.transpose(mm_nt(act, out_weight))
    rate = jax.nn.sigmoid(logit[0:1])
    both = rate * jax.nn.sigmoid(logit[1:2])
    for u in range(users):
        rate_ref[u : u + 1, :] = rate[:, u * cands : (u + 1) * cands]
        both_ref[u : u + 1, :] = both[:, u * cands : (u + 1) * cands]


def earlier_rows(length):
    return lax.div(length - 1, CHUNK) * CHUNK


def stage_kernel(from_ref, to_ref, sem_ref):
    copy = pltpu.make_async_copy(from_ref.at[pl.ds(0, to_ref.shape[0])], to_ref, sem_ref)
    copy.start()
    copy.wait()


def prepare_kernel(len_ref, slot_ref, history_ref, *refs):
    weights, (live_ref, pick_ref, last_ref), targets, sem_ref = refs[:3], refs[3:6], refs[6:9], refs[9]
    copies = [
        pltpu.make_async_copy(
            history_ref.at[u, pl.ds(pl.multiple_of(earlier_rows(len_ref[u]), CHUNK), CHUNK)],
            last_ref.at[u],
            sem_ref.at[u],
        )
        for u in range(history_ref.shape[0])
    ]
    copies += [
        pltpu.make_async_copy(source, target, sem_ref.at[history_ref.shape[0] + k])
        for k, (source, target) in enumerate(zip(weights, targets))
    ]
    for copy in copies:
        copy.start()
    for u in range(history_ref.shape[0]):
        live_ref[u : u + 1, :] = jnp.full((1, LANES), len_ref[u] - earlier_rows(len_ref[u]), jnp.int32)
    place = jnp.transpose(slot_ref[...])[:, 0:1]
    pick_ref[...] = ones_where(place == iota(pick_ref.shape, 1).astype(F32))
    for copy in copies:
        copy.wait()


def in_hbm(x):
    return pltpu.with_memory_space_constraint(x, pltpu.HBM)


def in_vmem(x):
    return pltpu.with_memory_space_constraint(x, pltpu.VMEM)


def window_cost(size):
    return pl.CostEstimate(flops=1 << 30, bytes_accessed=size, transcendentals=0)


def hbm():
    return pl.BlockSpec(memory_space=pltpu.HBM)


def limit(mib):
    return pltpu.CompilerParams(vmem_limit_bytes=mib << 20)


def vmem():
    return pl.BlockSpec(memory_space=pltpu.VMEM)


def local(
    history,
    lengths,
    candidates,
    item_table,
    value_weight,
    click_hidden,
    convert_hidden,
    click_output,
    convert_output,
):
    users, seq, width = history.shape
    cands = candidates.shape[1]
    table_rows, row_width = item_table.shape
    devices = lax.axis_size("gx") * lax.axis_size("gy")
    total = users * cands
    rows = HEADS * cands
    staged = 5 * table_rows // 8
    table = in_hbm(item_table)
    history = in_hbm(history)
    weights = (in_hbm(value_weight), in_hbm(click_hidden), in_hbm(convert_hidden))

    table_start = pl.pallas_call(
        stage_kernel,
        out_shape=pltpu.VMEM((staged, row_width), BF16),
        in_specs=[hbm()],
        out_specs=vmem(),
        scratch_shapes=[pltpu.SemaphoreType.DMA(())],
        cost_estimate=window_cost(2 * table.size),
        compiler_params=limit(2),
        name="stage",
    )(table)
    request, place = pl.pallas_call(
        functools.partial(request_kernel, owners=devices, row_bits=table_rows.bit_length() - 1),
        out_shape=(pltpu.VMEM((devices, LANES), F32), pltpu.VMEM((8, total), F32)),
        in_specs=[vmem()],
        out_specs=(vmem(), vmem()),
        compiler_params=limit(8),
        name="request",
    )(candidates)
    asked = lax.all_to_all(request, AXES, 0, 0, tiled=True)
    answer = pl.pallas_call(
        answer_kernel,
        out_shape=jax.ShapeDtypeStruct((devices * 16, LANES), BF16),
        in_specs=[vmem(), vmem(), hbm()],
        out_specs=vmem(),
        scratch_shapes=[
            pltpu.VMEM((devices * SLOTS, 256), BF16),
            pltpu.VMEM((devices * SLOTS, 256), BF16),
            pltpu.VMEM((devices * SLOTS, row_width), F32),
            pltpu.VMEM((table_rows - staged, row_width), BF16),
            pltpu.SemaphoreType.DMA(()),
        ],
        compiler_params=limit(24),
        name="answer",
    )(asked, in_vmem(table_start), table)
    answered = lax.all_to_all(answer, AXES, 0, 0, tiled=True)
    prepared = pl.pallas_call(
        prepare_kernel,
        out_shape=(
            pltpu.VMEM((users, LANES), jnp.int32),
            pltpu.VMEM((total, devices * SLOTS), BF16),
            pltpu.VMEM((users, CHUNK, width), BF16),
            *(pltpu.VMEM(w.shape, BF16) for w in weights),
        ),
        in_specs=[pl.BlockSpec(memory_space=pltpu.SMEM), vmem()] + [hbm()] * 4,
        out_specs=(vmem(),) * 6,
        scratch_shapes=[pltpu.SemaphoreType.DMA((users + 3,))],
        cost_estimate=window_cost(1 << 22),
        compiler_params=limit(4),
        name="prepare",
    )(lengths, place, history, *weights)
    live, pick, start, *weights = (in_vmem(x) for x in prepared)
    return pl.pallas_call(
        attend_kernel,
        out_shape=(
            jax.ShapeDtypeStruct((users, cands), F32),
            jax.ShapeDtypeStruct((users, cands), F32),
        ),
        in_specs=[hbm()] + [vmem()] * 7 + [hbm()] + [vmem()] * 2,
        out_specs=(vmem(), vmem()),
        scratch_shapes=[
            pltpu.VMEM((users, seq - CHUNK, width), BF16),
            pltpu.VMEM((users, rows, width), BF16),
            pltpu.VMEM((total, 3 * width), BF16),
            pltpu.VMEM((users + 1, rows, width), F32),
            pltpu.VMEM((users + 1, rows, LANES), F32),
            pltpu.VMEM((users + 1, rows, LANES), F32),
            *[pltpu.VMEM((rows, CHUNK), F32)] * 2,
            *[pltpu.VMEM((rows, CHUNK), BF16)] * 2,
            *[pltpu.VMEM((rows, LANES), F32)] * 2,
            pltpu.VMEM((2, total, click_hidden.shape[1]), F32),
            pltpu.SMEM((4, users * (seq // CHUNK - 1) + 7), jnp.int32),
            pltpu.SMEM((users,), jnp.int32),
            pltpu.SemaphoreType.DMA((users,)),
            pltpu.SemaphoreType.DMA(()),
        ],
        compiler_params=limit(24),
        name="attend",
    )(
        in_hbm(lengths),
        live,
        pick,
        answered,
        start,
        *weights,
        history,
        click_output.reshape(1, -1),
        convert_output.reshape(1, -1),
    )


def solution(mesh):
    split = P(AXES)
    return jax.shard_map(
        local,
        mesh=mesh,
        in_specs=(split, split, split, split, P(), P(), P(), P(), P()),
        out_specs=(split, split),
        check_vma=False,
    )
```

```python
import functools
import math

import jax
import jax.numpy as jnp
from jax import lax
from jax.experimental import pallas as pl
from jax.experimental.pallas import tpu as pltpu
from jax.sharding import PartitionSpec as P

HEADS = 4
SLOTS = 4
LANES = 128
CHUNK = 512
AXES = ("gx", "gy")
NEG = -1e30

F32 = jnp.float32
BF16 = jnp.bfloat16


def iota(shape, dim):
    return lax.broadcasted_iota(jnp.int32, shape, dim)


def ones_where(cond):
    return jnp.where(cond, 1.0, 0.0).astype(BF16)


def mm(a, b):
    return lax.dot_general(a, b, (((1,), (0,)), ((), ())), preferred_element_type=F32)


def mm_nt(a, b):
    return lax.dot_general(a, b, (((1,), (1,)), ((), ())), preferred_element_type=F32)


def request_kernel(cand_ref, req_ref, slot_ref, *, owners, row_bits):
    users, cands = cand_ref.shape
    total = users * cands
    ids = jnp.concatenate([cand_ref[u : u + 1, :] for u in range(users)], axis=1)
    owner = lax.shift_right_logical(ids, row_bits)
    row = jnp.bitwise_and(ids, (1 << row_bits) - 1)
    high = lax.shift_right_logical(row, 8).astype(F32)
    low = jnp.bitwise_and(row, 255).astype(F32)
    match = iota((owners, total), 0) == owner
    before = ones_where(iota((total, total), 0) < iota((total, total), 1))
    rank = mm(ones_where(match), before)
    place = jnp.sum(jnp.where(match, rank, 0.0), axis=0, keepdims=True) + (owner * SLOTS).astype(F32)
    slot_ref[...] = jnp.broadcast_to(place, slot_ref.shape)
    lane = iota((LANES, total), 0)
    picks, values = [], []
    for s in range(SLOTS):
        picks.append(ones_where(match & (rank == float(s))))
        values.append(
            jnp.where(lane == 2 * s, high, jnp.where(lane == 2 * s + 1, low, 0.0)).astype(BF16)
        )
    req_ref[...] = mm_nt(jnp.concatenate(picks, axis=1), jnp.concatenate(values, axis=1))


def answer_kernel(req_ref, staged_ref, table_ref, out_ref, hot_ref, high_ref, acc_ref, rest_ref, sem_ref):
    sources = req_ref.shape[0]
    rows = sources * SLOTS
    staged, width = staged_ref.shape
    rest = pltpu.make_async_copy(table_ref.at[pl.ds(staged, rest_ref.shape[0])], rest_ref, sem_ref)
    rest.start()
    spread = ones_where(lax.shift_right_logical(iota((rows, sources), 0), 2) == iota((rows, sources), 1))
    asked = mm(spread, req_ref[...].astype(BF16))
    own = lax.shift_right_logical(iota((rows, LANES), 1), 1) == jnp.bitwise_and(iota((rows, LANES), 0), 3)
    asked = jnp.where(own, asked, 0.0).astype(BF16)
    which = jnp.bitwise_and(iota((LANES, 512), 0), 1) == lax.shift_right_logical(iota((LANES, 512), 1), 8)
    both = mm(asked, ones_where(which))
    high_ref[...] = both[:, :256].astype(BF16)
    hot_ref[...] = ones_where(both[:, 256:] == iota((rows, 256), 1).astype(F32))

    def part(first, part_ref):
        hot = [
            jnp.where(high_ref[...] == jnp.array(first + k, BF16), hot_ref[...], jnp.zeros((), BF16))
            for k in range(part_ref.shape[0] // 256)
        ]
        return mm(jnp.concatenate(hot, axis=1), part_ref[...])

    acc_ref[...] = part(0, staged_ref)
    rest.wait()
    acc_ref[...] += part(staged // 256, rest_ref)
    quarter = [
        acc_ref[:, q * LANES : (q + 1) * LANES].reshape(rows // 8, 8, LANES) for q in range(width // LANES)
    ]
    first = iota((rows // 8, 8, LANES), 1) < 4

    def even(a, b):
        return jnp.where(first, a, pltpu.roll(b, 4, axis=1))

    def odd(a, b):
        return jnp.where(first, pltpu.roll(a, 4, axis=1), b)

    packed = jnp.concatenate(
        [
            even(quarter[0], quarter[1]),
            even(quarter[2], quarter[3]),
            odd(quarter[0], quarter[1]),
            odd(quarter[2], quarter[3]),
        ],
        axis=1,
    )
    out_ref[...] = packed.reshape(rows * 4, LANES).astype(BF16)


def attend_kernel(
    live_ref,
    pick_ref,
    answer_ref,
    last_ref,
    value_ref,
    click_ref,
    convert_ref,
    history_ref,
    click_out_ref,
    convert_out_ref,
    rate_ref,
    both_ref,
    hist_ref,
    query_ref,
    joined_ref,
    acc_ref,
    max_ref,
    sum_ref,
    score_a_ref,
    score_b_ref,
    weight_a_ref,
    weight_b_ref,
    scale_a_ref,
    scale_b_ref,
    early_ref,
    item_ref,
    len_ref,
    hist_sem,
):
    users, seq, width = history_ref.shape
    cands = rate_ref.shape[1]
    head_width = width // HEADS
    total = users * cands
    pieces = seq // CHUNK

    def rest(u):
        part = pl.ds(0, seq - CHUNK)
        return pltpu.make_async_copy(history_ref.at[u, part], hist_ref.at[u], hist_sem.at[u])

    for u in range(users):
        len_ref[u] = jnp.max(live_ref[users + u : users + u + 1, :]).astype(jnp.int32)

    group = answer_ref.shape[0] // 32
    got = answer_ref[...].astype(F32).reshape(group, 32, LANES)
    a0, b0, a1, b1 = (got[:, 8 * k : 8 * k + 8] for k in range(4))
    first = iota((group, 8, LANES), 1) < 4
    quarters = [
        jnp.where(first, a0, pltpu.roll(a1, 4, axis=1)),
        jnp.where(first, pltpu.roll(a0, 4, axis=1), a1),
        jnp.where(first, b0, pltpu.roll(b1, 4, axis=1)),
        jnp.where(first, pltpu.roll(b0, 4, axis=1), b1),
    ]
    answers = jnp.concatenate([q.reshape(group * 8, LANES).astype(BF16) for q in quarters], axis=1)
    rows_got = mm(pick_ref[...], answers)
    joined_ref[:, width:] = rows_got.astype(BF16)
    head_of_lane = lax.shift_right_logical(iota((cands, width), 1), head_width.bit_length() - 1)
    for u in range(users):
        target = rows_got[u * cands : (u + 1) * cands, :width] * (1.0 / math.sqrt(head_width))
        for h in range(HEADS):
            query_ref[u, h * cands : (h + 1) * cands, :] = jnp.where(
                head_of_lane == h, target, 0.0
            ).astype(BF16)


    def begin(u, carry):
        @pl.when(len_ref[u] > CHUNK)
        def _():
            rest(u).start()

        return carry

    lax.fori_loop(0, users, begin, 0)

    towers = (click_ref, convert_ref)
    for k, hidden in enumerate(towers):
        early_ref[k] = mm(joined_ref[:, width:], hidden[width:, :])
    lane = iota((1, CHUNK), 1)

    def exp_parts(scores_of, top):
        added = None
        weight = []
        for k in range(CHUNK // LANES):
            w = jnp.exp(scores_of(slice(k * LANES, (k + 1) * LANES)) - top)
            added = w if added is None else added + w
            weight.append(w.astype(BF16))
        return jnp.concatenate(weight, axis=1), added

    for u in range(users):
        block = last_ref[u]
        live = jnp.concatenate([live_ref[u : u + 1, :]] * (CHUNK // LANES), axis=1)
        scores = jnp.where(lane.astype(F32) < live, mm_nt(query_ref[u], block), NEG)
        top = jnp.broadcast_to(jnp.max(scores, axis=1, keepdims=True), (scores.shape[0], LANES))
        max_ref[u] = top
        weight, sum_ref[u] = exp_parts(lambda part: scores[:, part], top)
        acc_ref[u] = mm(weight, block)

    def enter(k, user, source, offset, wait):
        for field, value in enumerate((user, source, offset, wait)):
            item_ref[field, k] = value

    items = jnp.int32(0)
    for u in range(users):
        for j in range(1, pieces):

            @pl.when(len_ref[u] > j * CHUNK)
            def _():
                enter(items + (j + 1), u, u, (j - 1) * CHUNK, int(j == 1))

        items += lax.div(len_ref[u] - 1, CHUNK)
    for k in (0, 1, *(items + (k + 2) for k in range(5))):
        enter(k, users, 0, 0, 0)

    def entry(k):
        return tuple(item_ref[field, k] for field in range(4))

    def block(item):
        return hist_ref[item[1], pl.ds(pl.multiple_of(item[2], CHUNK), CHUNK), :]

    def step(now, ahead, beyond, score_to_ref, score_ref, weight_to_ref, scale_to_ref, weight_ref, scale_ref):
        score_to_ref[...] = mm_nt(query_ref[beyond[1]], block(beyond))

        u = ahead[0]
        old = max_ref[u]
        new = jnp.maximum(old, jnp.max(score_ref[...], axis=1, keepdims=True))
        scale = jnp.exp(old - new)
        max_ref[u] = new
        scale_to_ref[...] = scale
        weight_to_ref[...], added = exp_parts(lambda part: score_ref[:, part], new)
        sum_ref[u] = sum_ref[u] * scale + added

        u = now[0]
        context = mm(weight_ref[...], block(now))
        scale = scale_ref[...]
        for k in range(width // LANES):
            part = slice(k * LANES, (k + 1) * LANES)
            acc_ref[u, :, part] = acc_ref[u, :, part] * scale + context[:, part]

    def pair(p, carry):
        a, b, c, d = carry
        for item in (c, d):

            @pl.when(item[3] == 1)
            def _():
                rest(item[1]).wait()

        step(a, b, c, score_a_ref, score_b_ref, weight_b_ref, scale_b_ref, weight_a_ref, scale_a_ref)
        step(b, c, d, score_b_ref, score_a_ref, weight_a_ref, scale_a_ref, weight_b_ref, scale_b_ref)
        return c, d, entry(2 * p + 4), entry(2 * p + 5)

    @pl.when(items > 0)
    def _():
        lax.fori_loop(0, lax.div(items + 3, 2), pair, tuple(entry(k) for k in range(4)))

    row = iota((LANES, 1), 0)
    nothing = jnp.zeros((LANES, width), F32)
    click_out = jnp.where(row == 0, click_out_ref[...].astype(F32), nothing)
    convert_out = jnp.where(row == 1, convert_out_ref[...].astype(F32), nothing)
    out_weight = jnp.concatenate([click_out, convert_out], axis=1).astype(BF16)

    interest = []
    for u in range(users):
        context = acc_ref[u]
        coarse = context.astype(BF16)
        fine = (context - coarse.astype(F32)).astype(BF16)
        number = mm(coarse, value_ref[...]) + mm(fine, value_ref[...])
        above = jnp.zeros((cands, width), F32)
        below = jnp.ones((cands, width), F32)
        for h in range(HEADS):
            head = slice(h * cands, (h + 1) * cands)
            above = jnp.where(head_of_lane == h, number[head], above)
            below = jnp.where(head_of_lane == h, jnp.sum(sum_ref[u, head], axis=1, keepdims=True), below)
        pooled = above / below
        square = jnp.mean(pooled * pooled, axis=1, keepdims=True)
        interest.append((pooled * lax.rsqrt(square + 1e-06)).astype(BF16))
    act = []
    for u in range(0, users, 4):
        part = slice(u * cands, (u + 4) * cands)
        query = jnp.concatenate(interest[u : u + 4], axis=0)
        act.append(
            jnp.concatenate(
                [
                    jnp.maximum(mm(query, hidden[:width, :]) + early_ref[k, part], 0.0).astype(BF16)
                    for k, hidden in enumerate(towers)
                ],
                axis=1,
            )
        )
    act = jnp.concatenate(act, axis=0)
    logit = jnp.transpose(mm_nt(act, out_weight))
    rate = jax.nn.sigmoid(logit[0:1])
    both = rate * jax.nn.sigmoid(logit[1:2])
    for u in range(users):
        rate_ref[u : u + 1, :] = rate[:, u * cands : (u + 1) * cands]
        both_ref[u : u + 1, :] = both[:, u * cands : (u + 1) * cands]


def earlier_rows(length):
    return lax.div(length - 1, CHUNK) * CHUNK


def stage_kernel(from_ref, to_ref, sem_ref):
    copy = pltpu.make_async_copy(from_ref.at[pl.ds(0, to_ref.shape[0])], to_ref, sem_ref)
    copy.start()
    copy.wait()


def prepare_kernel(len_ref, slot_ref, history_ref, *refs):
    weights, (live_ref, pick_ref, last_ref), targets, sem_ref = refs[:3], refs[3:6], refs[6:9], refs[9]
    copies = [
        pltpu.make_async_copy(
            history_ref.at[u, pl.ds(pl.multiple_of(earlier_rows(len_ref[u]), CHUNK), CHUNK)],
            last_ref.at[u],
            sem_ref.at[u],
        )
        for u in range(history_ref.shape[0])
    ]
    copies += [
        pltpu.make_async_copy(source, target, sem_ref.at[history_ref.shape[0] + k])
        for k, (source, target) in enumerate(zip(weights, targets))
    ]
    for copy in copies:
        copy.start()
    users = history_ref.shape[0]
    for u in range(users):
        live = len_ref[u] - earlier_rows(len_ref[u])
        live_ref[u : u + 1, :] = jnp.full((1, LANES), live, jnp.int32).astype(F32)
        live_ref[users + u : users + u + 1, :] = jnp.full((1, LANES), len_ref[u], jnp.int32).astype(F32)
    place = jnp.transpose(slot_ref[...])[:, 0:1]
    pick_ref[...] = ones_where(place == iota(pick_ref.shape, 1).astype(F32))
    for copy in copies:
        copy.wait()


def in_hbm(x):
    return pltpu.with_memory_space_constraint(x, pltpu.HBM)


def in_vmem(x):
    return pltpu.with_memory_space_constraint(x, pltpu.VMEM)


def window_cost(size):
    return pl.CostEstimate(flops=1 << 30, bytes_accessed=size, transcendentals=0)


def hbm():
    return pl.BlockSpec(memory_space=pltpu.HBM)


def limit(mib):
    return pltpu.CompilerParams(vmem_limit_bytes=mib << 20)


def vmem():
    return pl.BlockSpec(memory_space=pltpu.VMEM)


def local(
    history,
    lengths,
    candidates,
    item_table,
    value_weight,
    click_hidden,
    convert_hidden,
    click_output,
    convert_output,
):
    users, seq, width = history.shape
    cands = candidates.shape[1]
    table_rows, row_width = item_table.shape
    devices = lax.axis_size("gx") * lax.axis_size("gy")
    total = users * cands
    rows = HEADS * cands
    staged = 5 * table_rows // 8
    table = in_hbm(item_table)
    history = in_hbm(history)
    weights = (in_hbm(value_weight), in_hbm(click_hidden), in_hbm(convert_hidden))

    table_start = pl.pallas_call(
        stage_kernel,
        out_shape=pltpu.VMEM((staged, row_width), BF16),
        in_specs=[hbm()],
        out_specs=vmem(),
        scratch_shapes=[pltpu.SemaphoreType.DMA(())],
        cost_estimate=window_cost(2 * table.size),
        compiler_params=limit(2),
        name="stage",
    )(table)
    request, place = pl.pallas_call(
        functools.partial(request_kernel, owners=devices, row_bits=table_rows.bit_length() - 1),
        out_shape=(pltpu.VMEM((devices, LANES), F32), pltpu.VMEM((8, total), F32)),
        in_specs=[vmem()],
        out_specs=(vmem(), vmem()),
        compiler_params=limit(8),
        name="request",
    )(candidates)
    asked = lax.all_to_all(request, AXES, 0, 0, tiled=True)
    answer = pl.pallas_call(
        answer_kernel,
        out_shape=jax.ShapeDtypeStruct((devices * 16, LANES), BF16),
        in_specs=[vmem(), vmem(), hbm()],
        out_specs=vmem(),
        scratch_shapes=[
            pltpu.VMEM((devices * SLOTS, 256), BF16),
            pltpu.VMEM((devices * SLOTS, 256), BF16),
            pltpu.VMEM((devices * SLOTS, row_width), F32),
            pltpu.VMEM((table_rows - staged, row_width), BF16),
            pltpu.SemaphoreType.DMA(()),
        ],
        compiler_params=limit(24),
        name="answer",
    )(asked, in_vmem(table_start), table)
    answered = lax.all_to_all(answer, AXES, 0, 0, tiled=True)
    prepared = pl.pallas_call(
        prepare_kernel,
        out_shape=(
            pltpu.VMEM((2 * users, LANES), F32),
            pltpu.VMEM((total, devices * SLOTS), BF16),
            pltpu.VMEM((users, CHUNK, width), BF16),
            *(pltpu.VMEM(w.shape, BF16) for w in weights),
        ),
        in_specs=[pl.BlockSpec(memory_space=pltpu.SMEM), vmem()] + [hbm()] * 4,
        out_specs=(vmem(),) * 6,
        scratch_shapes=[pltpu.SemaphoreType.DMA((users + 3,))],
        cost_estimate=window_cost(1 << 22),
        compiler_params=limit(4),
        name="prepare",
    )(lengths, place, history, *weights)
    live, pick, start, *weights = (in_vmem(x) for x in prepared)
    return pl.pallas_call(
        attend_kernel,
        out_shape=(
            jax.ShapeDtypeStruct((users, cands), F32),
            jax.ShapeDtypeStruct((users, cands), F32),
        ),
        in_specs=[vmem()] * 7 + [hbm()] + [vmem()] * 2,
        out_specs=(vmem(), vmem()),
        scratch_shapes=[
            pltpu.VMEM((users, seq - CHUNK, width), BF16),
            pltpu.VMEM((users, rows, width), BF16),
            pltpu.VMEM((total, 3 * width), BF16),
            pltpu.VMEM((users + 1, rows, width), F32),
            pltpu.VMEM((users + 1, rows, LANES), F32),
            pltpu.VMEM((users + 1, rows, LANES), F32),
            *[pltpu.VMEM((rows, CHUNK), F32)] * 2,
            *[pltpu.VMEM((rows, CHUNK), BF16)] * 2,
            *[pltpu.VMEM((rows, LANES), F32)] * 2,
            pltpu.VMEM((2, total, click_hidden.shape[1]), F32),
            pltpu.SMEM((4, users * (seq // CHUNK - 1) + 7), jnp.int32),
            pltpu.SMEM((users,), jnp.int32),
            pltpu.SemaphoreType.DMA((users,)),
        ],
        compiler_params=limit(24),
        name="attend",
    )(
        live,
        pick,
        answered,
        start,
        *weights,
        history,
        click_output.reshape(1, -1),
        convert_output.reshape(1, -1),
    )


def solution(mesh):
    split = P(AXES)
    return jax.shard_map(
        local,
        mesh=mesh,
        in_specs=(split, split, split, split, P(), P(), P(), P(), P()),
        out_specs=(split, split),
        check_vma=False,
    )
```

```python
import functools
import math

import jax
import jax.numpy as jnp
from jax import lax
from jax.experimental import pallas as pl
from jax.experimental.pallas import tpu as pltpu
from jax.sharding import PartitionSpec as P

HEADS = 4
SLOTS = 4
LANES = 128
CHUNK = 512
AXES = ("gx", "gy")
NEG = -1e30

F32 = jnp.float32
BF16 = jnp.bfloat16


def iota(shape, dim):
    return lax.broadcasted_iota(jnp.int32, shape, dim)


def ones_where(cond):
    return jnp.where(cond, 1.0, 0.0).astype(BF16)


def mm(a, b):
    return lax.dot_general(a, b, (((1,), (0,)), ((), ())), preferred_element_type=F32)


def mm_nt(a, b):
    return lax.dot_general(a, b, (((1,), (1,)), ((), ())), preferred_element_type=F32)


def request_kernel(cand_ref, req_ref, slot_ref, *, owners, row_bits):
    users, cands = cand_ref.shape
    total = users * cands
    ids = jnp.concatenate([cand_ref[u : u + 1, :] for u in range(users)], axis=1)
    owner = lax.shift_right_logical(ids, row_bits)
    row = jnp.bitwise_and(ids, (1 << row_bits) - 1)
    high = lax.shift_right_logical(row, 8).astype(F32)
    low = jnp.bitwise_and(row, 255).astype(F32)
    match = iota((owners, total), 0) == owner
    before = ones_where(iota((total, total), 0) < iota((total, total), 1))
    rank = mm(ones_where(match), before)
    place = jnp.sum(jnp.where(match, rank, 0.0), axis=0, keepdims=True) + (owner * SLOTS).astype(F32)
    slot_ref[...] = jnp.broadcast_to(place, slot_ref.shape)
    lane = iota((LANES, total), 0)
    picks, values = [], []
    for s in range(SLOTS):
        picks.append(ones_where(match & (rank == float(s))))
        values.append(
            jnp.where(lane == 2 * s, high, jnp.where(lane == 2 * s + 1, low, 0.0)).astype(BF16)
        )
    req_ref[...] = mm_nt(jnp.concatenate(picks, axis=1), jnp.concatenate(values, axis=1))


def answer_kernel(req_ref, staged_ref, table_ref, out_ref, hot_ref, high_ref, acc_ref, rest_ref, sem_ref):
    sources = req_ref.shape[0]
    rows = sources * SLOTS
    staged, width = staged_ref.shape
    rest = pltpu.make_async_copy(table_ref.at[pl.ds(staged, rest_ref.shape[0])], rest_ref, sem_ref)
    rest.start()
    spread = ones_where(lax.shift_right_logical(iota((rows, sources), 0), 2) == iota((rows, sources), 1))
    asked = mm(spread, req_ref[...].astype(BF16))
    own = lax.shift_right_logical(iota((rows, LANES), 1), 1) == jnp.bitwise_and(iota((rows, LANES), 0), 3)
    asked = jnp.where(own, asked, 0.0).astype(BF16)
    which = jnp.bitwise_and(iota((LANES, 512), 0), 1) == lax.shift_right_logical(iota((LANES, 512), 1), 8)
    both = mm(asked, ones_where(which))
    high_ref[...] = both[:, :256].astype(BF16)
    hot_ref[...] = ones_where(both[:, 256:] == iota((rows, 256), 1).astype(F32))

    def part(first, part_ref):
        hot = [
            jnp.where(high_ref[...] == jnp.array(first + k, BF16), hot_ref[...], jnp.zeros((), BF16))
            for k in range(part_ref.shape[0] // 256)
        ]
        return mm(jnp.concatenate(hot, axis=1), part_ref[...])

    acc_ref[...] = part(0, staged_ref)
    rest.wait()
    acc_ref[...] += part(staged // 256, rest_ref)
    quarter = [
        acc_ref[:, q * LANES : (q + 1) * LANES].reshape(rows // 8, 8, LANES) for q in range(width // LANES)
    ]
    first = iota((rows // 8, 8, LANES), 1) < 4

    def even(a, b):
        return jnp.where(first, a, pltpu.roll(b, 4, axis=1))

    def odd(a, b):
        return jnp.where(first, pltpu.roll(a, 4, axis=1), b)

    packed = jnp.concatenate(
        [
            even(quarter[0], quarter[1]),
            even(quarter[2], quarter[3]),
            odd(quarter[0], quarter[1]),
            odd(quarter[2], quarter[3]),
        ],
        axis=1,
    )
    out_ref[...] = packed.reshape(rows * 4, LANES).astype(BF16)


def attend_kernel(
    live_ref,
    pick_ref,
    answer_ref,
    last_ref,
    value_ref,
    click_ref,
    convert_ref,
    history_ref,
    click_out_ref,
    convert_out_ref,
    rate_ref,
    both_ref,
    hist_ref,
    query_ref,
    joined_ref,
    acc_ref,
    max_ref,
    sum_ref,
    score_a_ref,
    score_b_ref,
    weight_a_ref,
    weight_b_ref,
    scale_a_ref,
    scale_b_ref,
    early_ref,
    last_score_ref,
    item_ref,
    len_ref,
    hist_sem,
):
    users, seq, width = history_ref.shape
    cands = rate_ref.shape[1]
    head_width = width // HEADS
    total = users * cands
    pieces = seq // CHUNK

    def fetch(j):
        part = pl.ds(j * CHUNK, CHUNK)
        return pltpu.make_async_copy(history_ref.at[:, part], hist_ref.at[:, part], hist_sem.at[j])

    def begin(j, carry):
        fetch(j).start()
        return carry

    lax.fori_loop(0, pieces - 1, begin, 0)
    for u in range(users):
        len_ref[u] = jnp.max(live_ref[users + u : users + u + 1, :]).astype(jnp.int32)

    shift = pieces.bit_length() - 1
    idle = users * pieces
    waits = 2 * idle
    items = jnp.int32(0)
    met = []
    for j in range(pieces - 1):
        before = items
        for u in range(users):
            live = len_ref[u] > (j + 1) * CHUNK

            @pl.when(live)
            def _():
                item_ref[items] = u * pieces + j + jnp.where(items == before, waits, 0)

            items += live.astype(jnp.int32)
        met.append(items > before)
    for k in range(5):
        item_ref[items + k] = idle

    group = answer_ref.shape[0] // 32
    got = answer_ref[...].astype(F32).reshape(group, 32, LANES)
    a0, b0, a1, b1 = (got[:, 8 * k : 8 * k + 8] for k in range(4))
    first = iota((group, 8, LANES), 1) < 4
    quarters = [
        jnp.where(first, a0, pltpu.roll(a1, 4, axis=1)),
        jnp.where(first, pltpu.roll(a0, 4, axis=1), a1),
        jnp.where(first, b0, pltpu.roll(b1, 4, axis=1)),
        jnp.where(first, pltpu.roll(b0, 4, axis=1), b1),
    ]
    answers = jnp.concatenate([q.reshape(group * 8, LANES).astype(BF16) for q in quarters], axis=1)
    rows_got = mm(pick_ref[...], answers)
    joined_ref[:, width:] = rows_got.astype(BF16)
    head_of_lane = lax.shift_right_logical(iota((cands, width), 1), head_width.bit_length() - 1)
    for u in range(users):
        target = rows_got[u * cands : (u + 1) * cands, :width] * (1.0 / math.sqrt(head_width))
        for h in range(HEADS):
            query_ref[u, h * cands : (h + 1) * cands, :] = jnp.where(
                head_of_lane == h, target, 0.0
            ).astype(BF16)


    towers = (click_ref, convert_ref)
    lane = iota((1, CHUNK), 1)

    def exp_parts(scores_of, top):
        added = None
        weight = []
        for k in range(CHUNK // LANES):
            w = jnp.exp(scores_of(slice(k * LANES, (k + 1) * LANES)) - top)
            added = w if added is None else added + w
            weight.append(w.astype(BF16))
        return jnp.concatenate(weight, axis=1), added

    def last_score(u):
        live = jnp.concatenate([live_ref[u : u + 1, :]] * (CHUNK // LANES), axis=1)
        last_score_ref[u] = jnp.where(lane.astype(F32) < live, mm_nt(query_ref[u], last_ref[u]), NEG)

    last_score(0)
    for u in range(users):
        if u + 1 < users:
            last_score(u + 1)
        top = jnp.broadcast_to(jnp.max(last_score_ref[u], axis=1, keepdims=True), max_ref.shape[1:])
        max_ref[u] = top
        weight, sum_ref[u] = exp_parts(lambda part: last_score_ref[u, :, part], top)
        block = last_ref[u]
        acc_ref[u] = mm(weight, block)

    for k, hidden in enumerate(towers):
        early_ref[k] = mm(joined_ref[:, width:], hidden[width:, :])

    def entry(k):
        code = item_ref[k]
        user = lax.shift_right_logical(jnp.bitwise_and(code, waits - 1), shift)
        return (
            user,
            jnp.minimum(user, users - 1),
            jnp.bitwise_and(code, pieces - 1),
            (code >= waits).astype(jnp.int32),
        )

    def arrive(item):
        @pl.when(item[3] == 1)
        def _():
            fetch(item[2]).wait()

    def block(item):
        return hist_ref[item[1], pl.ds(pl.multiple_of(item[2] * CHUNK, CHUNK), CHUNK), :]

    def score(item, score_ref):
        score_ref[...] = mm_nt(query_ref[item[1]], block(item))

    def weigh(item, score_ref, weight_ref, scale_ref):
        u = item[0]
        old = max_ref[u]
        new = jnp.maximum(old, jnp.max(score_ref[...], axis=1, keepdims=True))
        scale = jnp.exp(old - new)
        max_ref[u] = new
        scale_ref[...] = scale
        weight_ref[...], added = exp_parts(lambda part: score_ref[:, part], new)
        sum_ref[u] = sum_ref[u] * scale + added

    def gather(item, weight_ref, scale_ref):
        u = item[0]
        context = mm(weight_ref[...], block(item))
        scale = scale_ref[...]
        for k in range(width // LANES):
            part = slice(k * LANES, (k + 1) * LANES)
            acc_ref[u, :, part] = acc_ref[u, :, part] * scale + context[:, part]

    def pair(p, carry):
        a, b, c, d = carry
        arrive(c)
        arrive(d)
        score(c, score_a_ref)
        weigh(b, score_b_ref, weight_b_ref, scale_b_ref)
        gather(a, weight_a_ref, scale_a_ref)
        score(d, score_b_ref)
        weigh(c, score_a_ref, weight_a_ref, scale_a_ref)
        gather(b, weight_b_ref, scale_b_ref)
        return c, d, entry(2 * p + 4), entry(2 * p + 5)

    @pl.when(items > 0)
    def _():
        begun = tuple(entry(k) for k in range(4))
        arrive(begun[0])
        arrive(begun[1])
        score(begun[0], score_a_ref)
        score(begun[1], score_b_ref)
        weigh(begun[0], score_a_ref, weight_a_ref, scale_a_ref)
        lax.fori_loop(0, lax.div(items + 1, 2) - 1, pair, begun)
        last = entry(items - 1)
        odd = jnp.bitwise_and(items, 1)

        @pl.when(odd == 1)
        def _():
            gather(last, weight_a_ref, scale_a_ref)

        @pl.when(odd == 0)
        def _():
            weigh(last, score_b_ref, weight_b_ref, scale_b_ref)
            gather(entry(items - 2), weight_a_ref, scale_a_ref)
            gather(last, weight_b_ref, scale_b_ref)

    row = iota((16, 1), 0)
    nothing = jnp.zeros((16, width), F32)
    click_out = jnp.where(row == 0, click_out_ref[...].astype(F32), nothing)
    convert_out = jnp.where(row == 1, convert_out_ref[...].astype(F32), nothing)
    out_weight = jnp.concatenate([click_out, convert_out], axis=1).astype(BF16)

    interest = []
    for u in range(users):
        context = acc_ref[u]
        coarse = context.astype(BF16)
        fine = (context - coarse.astype(F32)).astype(BF16)
        number = mm(coarse, value_ref[...]) + mm(fine, value_ref[...])
        above = jnp.zeros((cands, width), F32)
        below = jnp.ones((cands, width), F32)
        for h in range(HEADS):
            head = slice(h * cands, (h + 1) * cands)
            above = jnp.where(head_of_lane == h, number[head], above)
            below = jnp.where(head_of_lane == h, jnp.sum(sum_ref[u, head], axis=1, keepdims=True), below)
        pooled = above / below
        square = jnp.mean(pooled * pooled, axis=1, keepdims=True)
        interest.append((pooled * lax.rsqrt(square + 1e-06)).astype(BF16))
    act = []
    for u in range(0, users, 4):
        part = slice(u * cands, (u + 4) * cands)
        query = jnp.concatenate(interest[u : u + 4], axis=0)
        act.append(
            jnp.concatenate(
                [
                    jnp.maximum(mm(query, hidden[:width, :]) + early_ref[k, part], 0.0).astype(BF16)
                    for k, hidden in enumerate(towers)
                ],
                axis=1,
            )
        )
    act = jnp.concatenate(act, axis=0)
    for u in range(users):
        logit = mm_nt(out_weight, act[u * cands : (u + 1) * cands])
        chance = jax.nn.sigmoid(logit)
        rate_ref[u : u + 1, :] = chance[0:1]
        both_ref[u : u + 1, :] = chance[0:1] * chance[1:2]

    for j in range(pieces - 1):

        @pl.when(jnp.logical_not(met[j]))
        def _():
            fetch(j).wait()


def earlier_rows(length):
    return lax.div(length - 1, CHUNK) * CHUNK


def stage_kernel(from_ref, to_ref, sem_ref):
    copy = pltpu.make_async_copy(from_ref.at[pl.ds(0, to_ref.shape[0])], to_ref, sem_ref)
    copy.start()
    copy.wait()


def prepare_kernel(len_ref, slot_ref, history_ref, *refs):
    weights, (live_ref, pick_ref, last_ref), targets, sem_ref = refs[:3], refs[3:6], refs[6:9], refs[9]
    copies = [
        pltpu.make_async_copy(
            history_ref.at[u, pl.ds(pl.multiple_of(earlier_rows(len_ref[u]), CHUNK), CHUNK)],
            last_ref.at[u],
            sem_ref.at[u],
        )
        for u in range(history_ref.shape[0])
    ]
    copies += [
        pltpu.make_async_copy(source, target, sem_ref.at[history_ref.shape[0] + k])
        for k, (source, target) in enumerate(zip(weights, targets))
    ]
    for copy in copies:
        copy.start()
    users = history_ref.shape[0]
    for u in range(users):
        live = len_ref[u] - earlier_rows(len_ref[u])
        live_ref[u : u + 1, :] = jnp.full((1, LANES), live, jnp.int32).astype(F32)
        live_ref[users + u : users + u + 1, :] = jnp.full((1, LANES), len_ref[u], jnp.int32).astype(F32)
    place = jnp.transpose(slot_ref[...])[:, 0:1]
    pick_ref[...] = ones_where(place == iota(pick_ref.shape, 1).astype(F32))
    for copy in copies:
        copy.wait()


def in_hbm(x):
    return pltpu.with_memory_space_constraint(x, pltpu.HBM)


def in_vmem(x):
    return pltpu.with_memory_space_constraint(x, pltpu.VMEM)


def window_cost(size):
    return pl.CostEstimate(flops=1 << 30, bytes_accessed=size, transcendentals=0)


def hbm():
    return pl.BlockSpec(memory_space=pltpu.HBM)


def limit(mib):
    return pltpu.CompilerParams(vmem_limit_bytes=mib << 20)


def vmem():
    return pl.BlockSpec(memory_space=pltpu.VMEM)


def local(
    history,
    lengths,
    candidates,
    item_table,
    value_weight,
    click_hidden,
    convert_hidden,
    click_output,
    convert_output,
):
    users, seq, width = history.shape
    cands = candidates.shape[1]
    table_rows, row_width = item_table.shape
    devices = lax.axis_size("gx") * lax.axis_size("gy")
    total = users * cands
    rows = HEADS * cands
    staged = 5 * table_rows // 8
    table = in_hbm(item_table)
    history = in_hbm(history)
    weights = (in_hbm(value_weight), in_hbm(click_hidden), in_hbm(convert_hidden))

    table_start = pl.pallas_call(
        stage_kernel,
        out_shape=pltpu.VMEM((staged, row_width), BF16),
        in_specs=[hbm()],
        out_specs=vmem(),
        scratch_shapes=[pltpu.SemaphoreType.DMA(())],
        cost_estimate=window_cost(2 * table.size),
        compiler_params=limit(2),
        name="stage",
    )(table)
    request, place = pl.pallas_call(
        functools.partial(request_kernel, owners=devices, row_bits=table_rows.bit_length() - 1),
        out_shape=(pltpu.VMEM((devices, LANES), F32), pltpu.VMEM((8, total), F32)),
        in_specs=[vmem()],
        out_specs=(vmem(), vmem()),
        compiler_params=limit(8),
        name="request",
    )(candidates)
    asked = lax.all_to_all(request, AXES, 0, 0, tiled=True)
    answer = pl.pallas_call(
        answer_kernel,
        out_shape=jax.ShapeDtypeStruct((devices * 16, LANES), BF16),
        in_specs=[vmem(), vmem(), hbm()],
        out_specs=vmem(),
        scratch_shapes=[
            pltpu.VMEM((devices * SLOTS, 256), BF16),
            pltpu.VMEM((devices * SLOTS, 256), BF16),
            pltpu.VMEM((devices * SLOTS, row_width), F32),
            pltpu.VMEM((table_rows - staged, row_width), BF16),
            pltpu.SemaphoreType.DMA(()),
        ],
        compiler_params=limit(24),
        name="answer",
    )(asked, in_vmem(table_start), table)
    answered = lax.all_to_all(answer, AXES, 0, 0, tiled=True)
    prepared = pl.pallas_call(
        prepare_kernel,
        out_shape=(
            pltpu.VMEM((2 * users, LANES), F32),
            pltpu.VMEM((total, devices * SLOTS), BF16),
            pltpu.VMEM((users, CHUNK, width), BF16),
            *(pltpu.VMEM(w.shape, BF16) for w in weights),
        ),
        in_specs=[pl.BlockSpec(memory_space=pltpu.SMEM), vmem()] + [hbm()] * 4,
        out_specs=(vmem(),) * 6,
        scratch_shapes=[pltpu.SemaphoreType.DMA((users + 3,))],
        cost_estimate=window_cost(1 << 22),
        compiler_params=limit(4),
        name="prepare",
    )(lengths, place, history, *weights)
    live, pick, start, *weights = (in_vmem(x) for x in prepared)
    return pl.pallas_call(
        attend_kernel,
        out_shape=(
            jax.ShapeDtypeStruct((users, cands), F32),
            jax.ShapeDtypeStruct((users, cands), F32),
        ),
        in_specs=[vmem()] * 7 + [hbm()] + [vmem()] * 2,
        out_specs=(vmem(), vmem()),
        scratch_shapes=[
            pltpu.VMEM((users, seq - CHUNK, width), BF16),
            pltpu.VMEM((users, rows, width), BF16),
            pltpu.VMEM((total, 3 * width), BF16),
            pltpu.VMEM((users + 1, rows, width), F32),
            pltpu.VMEM((users + 1, rows, LANES), F32),
            pltpu.VMEM((users + 1, rows, LANES), F32),
            *[pltpu.VMEM((rows, CHUNK), F32)] * 2,
            *[pltpu.VMEM((rows, CHUNK), BF16)] * 2,
            *[pltpu.VMEM((rows, LANES), F32)] * 2,
            pltpu.VMEM((2, total, click_hidden.shape[1]), F32),
            pltpu.VMEM((users, rows, CHUNK), F32),
            pltpu.SMEM((users * (seq // CHUNK - 1) + 5,), jnp.int32),
            pltpu.SMEM((users,), jnp.int32),
            pltpu.SemaphoreType.DMA((seq // CHUNK - 1,)),
        ],
        compiler_params=limit(24),
        name="attend",
    )(
        live,
        pick,
        answered,
        start,
        *weights,
        history,
        click_output.reshape(1, -1),
        convert_output.reshape(1, -1),
    )


def solution(mesh):
    split = P(AXES)
    return jax.shard_map(
        local,
        mesh=mesh,
        in_specs=(split, split, split, split, P(), P(), P(), P(), P()),
        out_specs=(split, split),
        check_vma=False,
    )
```

```python
import functools
import math

import jax
import jax.numpy as jnp
from jax import lax
from jax.experimental import pallas as pl
from jax.experimental.pallas import tpu as pltpu
from jax.sharding import PartitionSpec as P

HEADS = 4
SLOTS = 4
LANES = 128
CHUNK = 512
AXES = ("gx", "gy")
NEG = -1e30

F32 = jnp.float32
BF16 = jnp.bfloat16


def iota(shape, dim):
    return lax.broadcasted_iota(jnp.int32, shape, dim)


def ones_where(cond):
    return jnp.where(cond, 1.0, 0.0).astype(BF16)


def mm(a, b):
    return lax.dot_general(a, b, (((1,), (0,)), ((), ())), preferred_element_type=F32)


def mm_nt(a, b):
    return lax.dot_general(a, b, (((1,), (1,)), ((), ())), preferred_element_type=F32)


def request_kernel(cand_ref, req_ref, slot_ref, *, owners, row_bits):
    users, cands = cand_ref.shape
    total = users * cands
    ids = jnp.concatenate([cand_ref[u : u + 1, :] for u in range(users)], axis=1)
    owner = lax.shift_right_logical(ids, row_bits)
    row = jnp.bitwise_and(ids, (1 << row_bits) - 1)
    high = lax.shift_right_logical(row, 8).astype(F32)
    low = jnp.bitwise_and(row, 255).astype(F32)
    match = iota((owners, total), 0) == owner
    before = ones_where(iota((total, total), 0) < iota((total, total), 1))
    rank = mm(ones_where(match), before)
    place = jnp.sum(jnp.where(match, rank, 0.0), axis=0, keepdims=True) + (owner * SLOTS).astype(F32)
    slot_ref[...] = jnp.broadcast_to(place, slot_ref.shape)
    lane = iota((LANES, total), 0)
    picks, values = [], []
    for s in range(SLOTS):
        picks.append(ones_where(match & (rank == float(s))))
        values.append(
            jnp.where(lane == 2 * s, high, jnp.where(lane == 2 * s + 1, low, 0.0)).astype(BF16)
        )
    req_ref[...] = mm_nt(jnp.concatenate(picks, axis=1), jnp.concatenate(values, axis=1))


def answer_kernel(req_ref, staged_ref, spread_ref, which_ref, table_ref, out_ref, hot_ref, high_ref, acc_ref, rest_ref, sem_ref):
    sources = req_ref.shape[0]
    rows = sources * SLOTS
    staged, width = staged_ref.shape
    rest = pltpu.make_async_copy(table_ref.at[pl.ds(staged, rest_ref.shape[0])], rest_ref, sem_ref)
    rest.start()
    asked = mm(spread_ref[...], req_ref[...].astype(BF16))
    own = lax.shift_right_logical(iota((rows, LANES), 1), 1) == jnp.bitwise_and(iota((rows, LANES), 0), 3)
    asked = jnp.where(own, asked, 0.0).astype(BF16)
    both = mm(asked, which_ref[...])
    high_ref[...] = both[:, :256].astype(BF16)
    hot_ref[...] = ones_where(both[:, 256:] == iota((rows, 256), 1).astype(F32))

    def part(first, part_ref):
        hot = [
            jnp.where(high_ref[...] == jnp.array(first + k, BF16), hot_ref[...], jnp.zeros((), BF16))
            for k in range(part_ref.shape[0] // 256)
        ]
        return mm(jnp.concatenate(hot, axis=1), part_ref[...])

    acc_ref[...] = part(0, staged_ref)
    rest.wait()
    acc_ref[...] += part(staged // 256, rest_ref)
    quarter = [
        acc_ref[:, q * LANES : (q + 1) * LANES].reshape(rows // 8, 8, LANES) for q in range(width // LANES)
    ]
    first = iota((rows // 8, 8, LANES), 1) < 4

    def even(a, b):
        return jnp.where(first, a, pltpu.roll(b, 4, axis=1))

    def odd(a, b):
        return jnp.where(first, pltpu.roll(a, 4, axis=1), b)

    packed = jnp.concatenate(
        [
            even(quarter[0], quarter[1]),
            even(quarter[2], quarter[3]),
            odd(quarter[0], quarter[1]),
            odd(quarter[2], quarter[3]),
        ],
        axis=1,
    )
    out_ref[...] = packed.reshape(rows * 4, LANES).astype(BF16)


def attend_kernel(
    live_ref,
    pick_ref,
    answer_ref,
    last_ref,
    value_ref,
    click_ref,
    convert_ref,
    history_ref,
    click_out_ref,
    convert_out_ref,
    rate_ref,
    both_ref,
    hist_ref,
    query_ref,
    joined_ref,
    acc_ref,
    max_ref,
    sum_ref,
    score_a_ref,
    score_b_ref,
    weight_a_ref,
    weight_b_ref,
    scale_a_ref,
    scale_b_ref,
    early_ref,
    last_score_ref,
    item_ref,
    len_ref,
    hist_sem,
):
    users, seq, width = history_ref.shape
    cands = rate_ref.shape[1]
    head_width = width // HEADS
    total = users * cands
    pieces = seq // CHUNK

    def fetch(j):
        part = pl.ds(j * CHUNK, CHUNK)
        return pltpu.make_async_copy(history_ref.at[:, part], hist_ref.at[:, part], hist_sem.at[j])

    def begin(j, carry):
        fetch(j).start()
        return carry

    lax.fori_loop(0, pieces - 1, begin, 0)
    for u in range(users):
        len_ref[u] = jnp.max(live_ref[users + u : users + u + 1, :]).astype(jnp.int32)

    shift = pieces.bit_length() - 1
    idle = users * pieces
    waits = 2 * idle
    items = jnp.int32(0)
    met = []
    for j in range(pieces - 1):
        before = items
        for u in range(users):
            live = len_ref[u] > (j + 1) * CHUNK

            @pl.when(live)
            def _():
                item_ref[items] = u * pieces + j + jnp.where(items == before, waits, 0)

            items += live.astype(jnp.int32)
        met.append(items > before)
    for k in range(5):
        item_ref[items + k] = idle

    group = answer_ref.shape[0] // 32
    got = answer_ref[...].astype(F32).reshape(group, 32, LANES)
    a0, b0, a1, b1 = (got[:, 8 * k : 8 * k + 8] for k in range(4))
    first = iota((group, 8, LANES), 1) < 4
    quarters = [
        jnp.where(first, a0, pltpu.roll(a1, 4, axis=1)),
        jnp.where(first, pltpu.roll(a0, 4, axis=1), a1),
        jnp.where(first, b0, pltpu.roll(b1, 4, axis=1)),
        jnp.where(first, pltpu.roll(b0, 4, axis=1), b1),
    ]
    answers = jnp.concatenate([q.reshape(group * 8, LANES).astype(BF16) for q in quarters], axis=1)
    rows_got = mm(pick_ref[...], answers)
    joined_ref[:, width:] = rows_got.astype(BF16)
    head_of_lane = lax.shift_right_logical(iota((cands, width), 1), head_width.bit_length() - 1)
    for u in range(users):
        target = rows_got[u * cands : (u + 1) * cands, :width] * (1.0 / math.sqrt(head_width))
        for h in range(HEADS):
            query_ref[u, h * cands : (h + 1) * cands, :] = jnp.where(
                head_of_lane == h, target, 0.0
            ).astype(BF16)


    towers = (click_ref, convert_ref)
    lane = iota((1, CHUNK), 1)

    def exp_parts(scores_of, top):
        added = None
        weight = []
        for k in range(CHUNK // LANES):
            w = jnp.exp(scores_of(slice(k * LANES, (k + 1) * LANES)) - top)
            added = w if added is None else added + w
            weight.append(w.astype(BF16))
        return jnp.concatenate(weight, axis=1), added

    def last_score(u):
        live = jnp.concatenate([live_ref[u : u + 1, :]] * (CHUNK // LANES), axis=1)
        last_score_ref[u] = jnp.where(lane.astype(F32) < live, mm_nt(query_ref[u], last_ref[u]), NEG)

    last_score(0)
    for u in range(users):
        if u + 1 < users:
            last_score(u + 1)
        top = jnp.broadcast_to(jnp.max(last_score_ref[u], axis=1, keepdims=True), max_ref.shape[1:])
        max_ref[u] = top
        weight, sum_ref[u] = exp_parts(lambda part: last_score_ref[u, :, part], top)
        block = last_ref[u]
        acc_ref[u] = mm(weight, block)

    for k, hidden in enumerate(towers):
        early_ref[k] = mm(joined_ref[:, width:], hidden[width:, :])

    def entry(k):
        code = item_ref[k]
        user = lax.shift_right_logical(jnp.bitwise_and(code, waits - 1), shift)
        return (
            user,
            jnp.minimum(user, users - 1),
            jnp.bitwise_and(code, pieces - 1),
            (code >= waits).astype(jnp.int32),
        )

    def arrive(item):
        @pl.when(item[3] == 1)
        def _():
            fetch(item[2]).wait()

    def block(item):
        return hist_ref[item[1], pl.ds(pl.multiple_of(item[2] * CHUNK, CHUNK), CHUNK), :]

    def score(item, score_ref):
        score_ref[...] = mm_nt(query_ref[item[1]], block(item))

    def weigh(item, score_ref, weight_ref, scale_ref):
        u = item[0]
        old = max_ref[u]
        new = jnp.maximum(old, jnp.max(score_ref[...], axis=1, keepdims=True))
        scale = jnp.exp(old - new)
        max_ref[u] = new
        scale_ref[...] = scale
        weight_ref[...], added = exp_parts(lambda part: score_ref[:, part], new)
        sum_ref[u] = sum_ref[u] * scale + added

    def gather(item, weight_ref, scale_ref):
        u = item[0]
        context = mm(weight_ref[...], block(item))
        scale = scale_ref[...]
        for k in range(width // LANES):
            part = slice(k * LANES, (k + 1) * LANES)
            acc_ref[u, :, part] = acc_ref[u, :, part] * scale + context[:, part]

    def pair(p, carry):
        a, b, c, d = carry
        arrive(c)
        arrive(d)
        score(c, score_a_ref)
        weigh(b, score_b_ref, weight_b_ref, scale_b_ref)
        gather(a, weight_a_ref, scale_a_ref)
        score(d, score_b_ref)
        weigh(c, score_a_ref, weight_a_ref, scale_a_ref)
        gather(b, weight_b_ref, scale_b_ref)
        return c, d, entry(2 * p + 4), entry(2 * p + 5)

    @pl.when(items > 0)
    def _():
        begun = tuple(entry(k) for k in range(4))
        arrive(begun[0])
        arrive(begun[1])
        score(begun[0], score_a_ref)
        score(begun[1], score_b_ref)
        weigh(begun[0], score_a_ref, weight_a_ref, scale_a_ref)
        lax.fori_loop(0, lax.div(items + 1, 2) - 1, pair, begun)
        last = entry(items - 1)
        odd = jnp.bitwise_and(items, 1)

        @pl.when(odd == 1)
        def _():
            gather(last, weight_a_ref, scale_a_ref)

        @pl.when(odd == 0)
        def _():
            weigh(last, score_b_ref, weight_b_ref, scale_b_ref)
            gather(entry(items - 2), weight_a_ref, scale_a_ref)
            gather(last, weight_b_ref, scale_b_ref)

    row = iota((16, 1), 0)
    nothing = jnp.zeros((16, width), F32)
    click_out = jnp.where(row == 0, click_out_ref[...].astype(F32), nothing)
    convert_out = jnp.where(row == 1, convert_out_ref[...].astype(F32), nothing)
    out_weight = jnp.concatenate([click_out, convert_out], axis=1).astype(BF16)

    interest = []
    for u in range(users):
        context = acc_ref[u]
        coarse = context.astype(BF16)
        fine = (context - coarse.astype(F32)).astype(BF16)
        number = mm(coarse, value_ref[...]) + mm(fine, value_ref[...])
        above = jnp.zeros((cands, width), F32)
        below = jnp.ones((cands, width), F32)
        for h in range(HEADS):
            head = slice(h * cands, (h + 1) * cands)
            above = jnp.where(head_of_lane == h, number[head], above)
            below = jnp.where(head_of_lane == h, jnp.sum(sum_ref[u, head], axis=1, keepdims=True), below)
        pooled = above / below
        square = jnp.mean(pooled * pooled, axis=1, keepdims=True)
        interest.append((pooled * lax.rsqrt(square + 1e-06)).astype(BF16))
    act = []
    for u in range(0, users, 4):
        part = slice(u * cands, (u + 4) * cands)
        query = jnp.concatenate(interest[u : u + 4], axis=0)
        act.append(
            jnp.concatenate(
                [
                    jnp.maximum(mm(query, hidden[:width, :]) + early_ref[k, part], 0.0).astype(BF16)
                    for k, hidden in enumerate(towers)
                ],
                axis=1,
            )
        )
    act = jnp.concatenate(act, axis=0)
    for u in range(users):
        logit = mm_nt(out_weight, act[u * cands : (u + 1) * cands])
        chance = jax.nn.sigmoid(logit)
        rate_ref[u : u + 1, :] = chance[0:1]
        both_ref[u : u + 1, :] = chance[0:1] * chance[1:2]

    for j in range(pieces - 1):

        @pl.when(jnp.logical_not(met[j]))
        def _():
            fetch(j).wait()


def earlier_rows(length):
    return lax.div(length - 1, CHUNK) * CHUNK


def stage_kernel(from_ref, to_ref, spread_ref, which_ref, sem_ref):
    copy = pltpu.make_async_copy(from_ref.at[pl.ds(0, to_ref.shape[0])], to_ref, sem_ref)
    copy.start()
    shape = spread_ref.shape
    spread_ref[...] = ones_where(lax.shift_right_logical(iota(shape, 0), 2) == iota(shape, 1))
    shape = which_ref.shape
    which = jnp.bitwise_and(iota(shape, 0), 1) == lax.shift_right_logical(iota(shape, 1), 8)
    which_ref[...] = ones_where(which)
    copy.wait()


def prepare_kernel(len_ref, slot_ref, history_ref, *refs):
    weights, (live_ref, pick_ref, last_ref), targets, sem_ref = refs[:3], refs[3:6], refs[6:9], refs[9]
    copies = [
        pltpu.make_async_copy(
            history_ref.at[u, pl.ds(pl.multiple_of(earlier_rows(len_ref[u]), CHUNK), CHUNK)],
            last_ref.at[u],
            sem_ref.at[u],
        )
        for u in range(history_ref.shape[0])
    ]
    copies += [
        pltpu.make_async_copy(source, target, sem_ref.at[history_ref.shape[0] + k])
        for k, (source, target) in enumerate(zip(weights, targets))
    ]
    for copy in copies:
        copy.start()
    users = history_ref.shape[0]
    for u in range(users):
        live = len_ref[u] - earlier_rows(len_ref[u])
        live_ref[u : u + 1, :] = jnp.full((1, LANES), live, jnp.int32).astype(F32)
        live_ref[users + u : users + u + 1, :] = jnp.full((1, LANES), len_ref[u], jnp.int32).astype(F32)
    place = jnp.transpose(slot_ref[...])[:, 0:1]
    pick_ref[...] = ones_where(place == iota(pick_ref.shape, 1).astype(F32))
    for copy in copies:
        copy.wait()


def in_hbm(x):
    return pltpu.with_memory_space_constraint(x, pltpu.HBM)


def in_vmem(x):
    return pltpu.with_memory_space_constraint(x, pltpu.VMEM)


def window_cost(size):
    return pl.CostEstimate(flops=1 << 30, bytes_accessed=size, transcendentals=0)


def hbm():
    return pl.BlockSpec(memory_space=pltpu.HBM)


def limit(mib):
    return pltpu.CompilerParams(vmem_limit_bytes=mib << 20)


def vmem():
    return pl.BlockSpec(memory_space=pltpu.VMEM)


def local(
    history,
    lengths,
    candidates,
    item_table,
    value_weight,
    click_hidden,
    convert_hidden,
    click_output,
    convert_output,
):
    users, seq, width = history.shape
    cands = candidates.shape[1]
    table_rows, row_width = item_table.shape
    devices = lax.axis_size("gx") * lax.axis_size("gy")
    total = users * cands
    rows = HEADS * cands
    staged = 5 * table_rows // 8
    table = in_hbm(item_table)
    history = in_hbm(history)
    weights = (in_hbm(value_weight), in_hbm(click_hidden), in_hbm(convert_hidden))

    table_start = pl.pallas_call(
        stage_kernel,
        out_shape=(
            pltpu.VMEM((staged, row_width), BF16),
            pltpu.VMEM((devices * SLOTS, devices), BF16),
            pltpu.VMEM((LANES, 512), BF16),
        ),
        in_specs=[hbm()],
        out_specs=(vmem(),) * 3,
        scratch_shapes=[pltpu.SemaphoreType.DMA(())],
        cost_estimate=window_cost(2 * table.size),
        compiler_params=limit(2),
        name="stage",
    )(table)
    request, place = pl.pallas_call(
        functools.partial(request_kernel, owners=devices, row_bits=table_rows.bit_length() - 1),
        out_shape=(pltpu.VMEM((devices, LANES), F32), pltpu.VMEM((8, total), F32)),
        in_specs=[vmem()],
        out_specs=(vmem(), vmem()),
        compiler_params=limit(8),
        name="request",
    )(candidates)
    asked = lax.all_to_all(request, AXES, 0, 0, tiled=True)
    answer = pl.pallas_call(
        answer_kernel,
        out_shape=jax.ShapeDtypeStruct((devices * 16, LANES), BF16),
        in_specs=[vmem()] * 4 + [hbm()],
        out_specs=vmem(),
        scratch_shapes=[
            pltpu.VMEM((devices * SLOTS, 256), BF16),
            pltpu.VMEM((devices * SLOTS, 256), BF16),
            pltpu.VMEM((devices * SLOTS, row_width), F32),
            pltpu.VMEM((table_rows - staged, row_width), BF16),
            pltpu.SemaphoreType.DMA(()),
        ],
        compiler_params=limit(24),
        name="answer",
    )(asked, *(in_vmem(x) for x in table_start), table)
    answered = lax.all_to_all(answer, AXES, 0, 0, tiled=True)
    prepared = pl.pallas_call(
        prepare_kernel,
        out_shape=(
            pltpu.VMEM((2 * users, LANES), F32),
            pltpu.VMEM((total, devices * SLOTS), BF16),
            pltpu.VMEM((users, CHUNK, width), BF16),
            *(pltpu.VMEM(w.shape, BF16) for w in weights),
        ),
        in_specs=[pl.BlockSpec(memory_space=pltpu.SMEM), vmem()] + [hbm()] * 4,
        out_specs=(vmem(),) * 6,
        scratch_shapes=[pltpu.SemaphoreType.DMA((users + 3,))],
        cost_estimate=window_cost(1 << 22),
        compiler_params=limit(4),
        name="prepare",
    )(lengths, place, history, *weights)
    live, pick, start, *weights = (in_vmem(x) for x in prepared)
    return pl.pallas_call(
        attend_kernel,
        out_shape=(
            jax.ShapeDtypeStruct((users, cands), F32),
            jax.ShapeDtypeStruct((users, cands), F32),
        ),
        in_specs=[vmem()] * 7 + [hbm()] + [vmem()] * 2,
        out_specs=(vmem(), vmem()),
        scratch_shapes=[
            pltpu.VMEM((users, seq - CHUNK, width), BF16),
            pltpu.VMEM((users, rows, width), BF16),
            pltpu.VMEM((total, 3 * width), BF16),
            pltpu.VMEM((users + 1, rows, width), F32),
            pltpu.VMEM((users + 1, rows, LANES), F32),
            pltpu.VMEM((users + 1, rows, LANES), F32),
            *[pltpu.VMEM((rows, CHUNK), F32)] * 2,
            *[pltpu.VMEM((rows, CHUNK), BF16)] * 2,
            *[pltpu.VMEM((rows, LANES), F32)] * 2,
            pltpu.VMEM((2, total, click_hidden.shape[1]), F32),
            pltpu.VMEM((users, rows, CHUNK), F32),
            pltpu.SMEM((users * (seq // CHUNK - 1) + 5,), jnp.int32),
            pltpu.SMEM((users,), jnp.int32),
            pltpu.SemaphoreType.DMA((seq // CHUNK - 1,)),
        ],
        compiler_params=limit(24),
        name="attend",
    )(
        live,
        pick,
        answered,
        start,
        *weights,
        history,
        click_output.reshape(1, -1),
        convert_output.reshape(1, -1),
    )


def solution(mesh):
    split = P(AXES)
    return jax.shard_map(
        local,
        mesh=mesh,
        in_specs=(split, split, split, split, P(), P(), P(), P(), P()),
        out_specs=(split, split),
        check_vma=False,
    )
```

```python
import functools
import math

import jax
import jax.numpy as jnp
from jax import lax
from jax.experimental import pallas as pl
from jax.experimental.pallas import tpu as pltpu
from jax.sharding import PartitionSpec as P

HEADS = 4
SLOTS = 4
LANES = 128
CHUNK = 512
AXES = ("gx", "gy")
NEG = -1e30

F32 = jnp.float32
BF16 = jnp.bfloat16


def iota(shape, dim):
    return lax.broadcasted_iota(jnp.int32, shape, dim)


def ones_where(cond):
    return jnp.where(cond, 1.0, 0.0).astype(BF16)


def mm(a, b):
    return lax.dot_general(a, b, (((1,), (0,)), ((), ())), preferred_element_type=F32)


def mm_nt(a, b):
    return lax.dot_general(a, b, (((1,), (1,)), ((), ())), preferred_element_type=F32)


def request_kernel(cand_hbm_ref, req_ref, slot_ref, cand_ref, before_ref, sem_ref, *, owners, row_bits):
    users, cands = cand_ref.shape
    total = users * cands
    arrival = pltpu.make_async_copy(cand_hbm_ref, cand_ref, sem_ref)
    arrival.start()
    before_ref[...] = ones_where(iota((total, total), 0) < iota((total, total), 1))
    arrival.wait()
    ids = jnp.concatenate([cand_ref[u : u + 1, :] for u in range(users)], axis=1)
    owner = lax.shift_right_logical(ids, row_bits)
    row = jnp.bitwise_and(ids, (1 << row_bits) - 1)
    high = lax.shift_right_logical(row, 8).astype(F32)
    low = jnp.bitwise_and(row, 255).astype(F32)
    match = iota((owners, total), 0) == owner
    rank = mm(ones_where(match), before_ref[...])
    place = jnp.sum(jnp.where(match, rank, 0.0), axis=0, keepdims=True) + (owner * SLOTS).astype(F32)
    slot_ref[...] = jnp.broadcast_to(place, slot_ref.shape)
    lane = iota((LANES, total), 0)
    picks, values = [], []
    for s in range(SLOTS):
        picks.append(ones_where(match & (rank == float(s))))
        values.append(
            jnp.where(lane == 2 * s, high, jnp.where(lane == 2 * s + 1, low, 0.0)).astype(BF16)
        )
    req_ref[...] = mm_nt(jnp.concatenate(picks, axis=1), jnp.concatenate(values, axis=1))


def answer_kernel(req_ref, staged_ref, table_ref, out_ref, hot_ref, high_ref, acc_ref, rest_ref, sem_ref):
    sources = req_ref.shape[0]
    rows = sources * SLOTS
    staged, width = staged_ref.shape
    rest = pltpu.make_async_copy(table_ref.at[pl.ds(staged, rest_ref.shape[0])], rest_ref, sem_ref)
    rest.start()
    spread = ones_where(lax.shift_right_logical(iota((rows, sources), 0), 2) == iota((rows, sources), 1))
    asked = mm(spread, req_ref[...].astype(BF16))
    own = lax.shift_right_logical(iota((rows, LANES), 1), 1) == jnp.bitwise_and(iota((rows, LANES), 0), 3)
    asked = jnp.where(own, asked, 0.0).astype(BF16)
    which = jnp.bitwise_and(iota((LANES, 512), 0), 1) == lax.shift_right_logical(iota((LANES, 512), 1), 8)
    both = mm(asked, ones_where(which))
    high_ref[...] = both[:, :256].astype(BF16)
    hot_ref[...] = ones_where(both[:, 256:] == iota((rows, 256), 1).astype(F32))

    def part(first, part_ref):
        hot = [
            jnp.where(high_ref[...] == jnp.array(first + k, BF16), hot_ref[...], jnp.zeros((), BF16))
            for k in range(part_ref.shape[0] // 256)
        ]
        return mm(jnp.concatenate(hot, axis=1), part_ref[...])

    acc_ref[...] = part(0, staged_ref)
    rest.wait()
    acc_ref[...] += part(staged // 256, rest_ref)
    quarter = [
        acc_ref[:, q * LANES : (q + 1) * LANES].reshape(rows // 8, 8, LANES) for q in range(width // LANES)
    ]
    first = iota((rows // 8, 8, LANES), 1) < 4

    def even(a, b):
        return jnp.where(first, a, pltpu.roll(b, 4, axis=1))

    def odd(a, b):
        return jnp.where(first, pltpu.roll(a, 4, axis=1), b)

    packed = jnp.concatenate(
        [
            even(quarter[0], quarter[1]),
            even(quarter[2], quarter[3]),
            odd(quarter[0], quarter[1]),
            odd(quarter[2], quarter[3]),
        ],
        axis=1,
    )
    out_ref[...] = packed.reshape(rows * 4, LANES).astype(BF16)


def attend_kernel(
    live_ref,
    pick_ref,
    answer_ref,
    last_ref,
    value_ref,
    click_ref,
    convert_ref,
    history_ref,
    click_out_ref,
    convert_out_ref,
    rate_ref,
    both_ref,
    hist_ref,
    query_ref,
    joined_ref,
    acc_ref,
    max_ref,
    sum_ref,
    score_a_ref,
    score_b_ref,
    weight_a_ref,
    weight_b_ref,
    scale_a_ref,
    scale_b_ref,
    early_ref,
    last_score_ref,
    item_ref,
    len_ref,
    hist_sem,
):
    users, seq, width = history_ref.shape
    cands = rate_ref.shape[1]
    head_width = width // HEADS
    total = users * cands
    pieces = seq // CHUNK

    def fetch(j):
        part = pl.ds(j * CHUNK, CHUNK)
        return pltpu.make_async_copy(history_ref.at[:, part], hist_ref.at[:, part], hist_sem.at[j])

    def begin(j, carry):
        fetch(j).start()
        return carry

    lax.fori_loop(0, pieces - 1, begin, 0)
    for u in range(users):
        len_ref[u] = jnp.max(live_ref[users + u : users + u + 1, :]).astype(jnp.int32)

    shift = pieces.bit_length() - 1
    idle = users * pieces
    waits = 2 * idle
    items = jnp.int32(0)
    met = []
    for j in range(pieces - 1):
        before = items
        for u in range(users):
            live = len_ref[u] > (j + 1) * CHUNK

            @pl.when(live)
            def _():
                item_ref[items] = u * pieces + j + jnp.where(items == before, waits, 0)

            items += live.astype(jnp.int32)
        met.append(items > before)
    for k in range(5):
        item_ref[items + k] = idle

    group = answer_ref.shape[0] // 32
    got = answer_ref[...].astype(F32).reshape(group, 32, LANES)
    a0, b0, a1, b1 = (got[:, 8 * k : 8 * k + 8] for k in range(4))
    first = iota((group, 8, LANES), 1) < 4
    quarters = [
        jnp.where(first, a0, pltpu.roll(a1, 4, axis=1)),
        jnp.where(first, pltpu.roll(a0, 4, axis=1), a1),
        jnp.where(first, b0, pltpu.roll(b1, 4, axis=1)),
        jnp.where(first, pltpu.roll(b0, 4, axis=1), b1),
    ]
    answers = jnp.concatenate([q.reshape(group * 8, LANES).astype(BF16) for q in quarters], axis=1)
    rows_got = mm(pick_ref[...], answers)
    joined_ref[:, width:] = rows_got.astype(BF16)
    head_of_lane = lax.shift_right_logical(iota((cands, width), 1), head_width.bit_length() - 1)
    for u in range(users):
        target = rows_got[u * cands : (u + 1) * cands, :width] * (1.0 / math.sqrt(head_width))
        for h in range(HEADS):
            query_ref[u, h * cands : (h + 1) * cands, :] = jnp.where(
                head_of_lane == h, target, 0.0
            ).astype(BF16)


    towers = (click_ref, convert_ref)
    lane = iota((1, CHUNK), 1)

    def exp_parts(scores_of, top):
        added = None
        weight = []
        for k in range(CHUNK // LANES):
            w = jnp.exp(scores_of(slice(k * LANES, (k + 1) * LANES)) - top)
            added = w if added is None else added + w
            weight.append(w.astype(BF16))
        return jnp.concatenate(weight, axis=1), added

    def last_score(u):
        live = jnp.concatenate([live_ref[u : u + 1, :]] * (CHUNK // LANES), axis=1)
        last_score_ref[u] = jnp.where(lane.astype(F32) < live, mm_nt(query_ref[u], last_ref[u]), NEG)

    last_score(0)
    for u in range(users):
        if u + 1 < users:
            last_score(u + 1)
        top = jnp.broadcast_to(jnp.max(last_score_ref[u], axis=1, keepdims=True), max_ref.shape[1:])
        max_ref[u] = top
        weight, sum_ref[u] = exp_parts(lambda part: last_score_ref[u, :, part], top)
        block = last_ref[u]
        acc_ref[u] = mm(weight, block)

    for k, hidden in enumerate(towers):
        early_ref[k] = mm(joined_ref[:, width:], hidden[width:, :])

    def entry(k):
        code = item_ref[k]
        user = lax.shift_right_logical(jnp.bitwise_and(code, waits - 1), shift)
        return (
            user,
            jnp.minimum(user, users - 1),
            jnp.bitwise_and(code, pieces - 1),
            (code >= waits).astype(jnp.int32),
        )

    def arrive(item):
        @pl.when(item[3] == 1)
        def _():
            fetch(item[2]).wait()

    def block(item):
        return hist_ref[item[1], pl.ds(pl.multiple_of(item[2] * CHUNK, CHUNK), CHUNK), :]

    def score(item, score_ref):
        score_ref[...] = mm_nt(query_ref[item[1]], block(item))

    def weigh(item, score_ref, weight_ref, scale_ref):
        u = item[0]
        old = max_ref[u]
        new = jnp.maximum(old, jnp.max(score_ref[...], axis=1, keepdims=True))
        scale = jnp.exp(old - new)
        max_ref[u] = new
        scale_ref[...] = scale
        weight_ref[...], added = exp_parts(lambda part: score_ref[:, part], new)
        sum_ref[u] = sum_ref[u] * scale + added

    def gather(item, weight_ref, scale_ref):
        u = item[0]
        context = mm(weight_ref[...], block(item))
        scale = scale_ref[...]
        for k in range(width // LANES):
            part = slice(k * LANES, (k + 1) * LANES)
            acc_ref[u, :, part] = acc_ref[u, :, part] * scale + context[:, part]

    def pair(p, carry):
        a, b, c, d = carry
        arrive(c)
        arrive(d)
        score(c, score_a_ref)
        weigh(b, score_b_ref, weight_b_ref, scale_b_ref)
        gather(a, weight_a_ref, scale_a_ref)
        score(d, score_b_ref)
        weigh(c, score_a_ref, weight_a_ref, scale_a_ref)
        gather(b, weight_b_ref, scale_b_ref)
        return c, d, entry(2 * p + 4), entry(2 * p + 5)

    @pl.when(items > 0)
    def _():
        begun = tuple(entry(k) for k in range(4))
        arrive(begun[0])
        arrive(begun[1])
        score(begun[0], score_a_ref)
        score(begun[1], score_b_ref)
        weigh(begun[0], score_a_ref, weight_a_ref, scale_a_ref)
        lax.fori_loop(0, lax.div(items + 1, 2) - 1, pair, begun)
        last = entry(items - 1)
        odd = jnp.bitwise_and(items, 1)

        @pl.when(odd == 1)
        def _():
            gather(last, weight_a_ref, scale_a_ref)

        @pl.when(odd == 0)
        def _():
            weigh(last, score_b_ref, weight_b_ref, scale_b_ref)
            gather(entry(items - 2), weight_a_ref, scale_a_ref)
            gather(last, weight_b_ref, scale_b_ref)

    row = iota((16, 1), 0)
    nothing = jnp.zeros((16, width), F32)
    click_out = jnp.where(row == 0, click_out_ref[...].astype(F32), nothing)
    convert_out = jnp.where(row == 1, convert_out_ref[...].astype(F32), nothing)
    out_weight = jnp.concatenate([click_out, convert_out], axis=1).astype(BF16)

    interest = []
    for u in range(users):
        context = acc_ref[u]
        coarse = context.astype(BF16)
        fine = (context - coarse.astype(F32)).astype(BF16)
        number = mm(coarse, value_ref[...]) + mm(fine, value_ref[...])
        above = jnp.zeros((cands, width), F32)
        below = jnp.ones((cands, width), F32)
        for h in range(HEADS):
            head = slice(h * cands, (h + 1) * cands)
            above = jnp.where(head_of_lane == h, number[head], above)
            below = jnp.where(head_of_lane == h, jnp.sum(sum_ref[u, head], axis=1, keepdims=True), below)
        pooled = above / below
        square = jnp.mean(pooled * pooled, axis=1, keepdims=True)
        interest.append((pooled * lax.rsqrt(square + 1e-06)).astype(BF16))
    act = []
    for u in range(0, users, 4):
        part = slice(u * cands, (u + 4) * cands)
        query = jnp.concatenate(interest[u : u + 4], axis=0)
        act.append(
            jnp.concatenate(
                [
                    jnp.maximum(mm(query, hidden[:width, :]) + early_ref[k, part], 0.0).astype(BF16)
                    for k, hidden in enumerate(towers)
                ],
                axis=1,
            )
        )
    act = jnp.concatenate(act, axis=0)
    for u in range(users):
        logit = mm_nt(out_weight, act[u * cands : (u + 1) * cands])
        chance = jax.nn.sigmoid(logit)
        rate_ref[u : u + 1, :] = chance[0:1]
        both_ref[u : u + 1, :] = chance[0:1] * chance[1:2]

    for j in range(pieces - 1):

        @pl.when(jnp.logical_not(met[j]))
        def _():
            fetch(j).wait()


def earlier_rows(length):
    return lax.div(length - 1, CHUNK) * CHUNK


def stage_kernel(from_ref, to_ref, sem_ref):
    copy = pltpu.make_async_copy(from_ref.at[pl.ds(0, to_ref.shape[0])], to_ref, sem_ref)
    copy.start()
    copy.wait()


def prepare_kernel(len_ref, slot_ref, history_ref, *refs):
    weights, (live_ref, pick_ref, last_ref), targets, sem_ref = refs[:3], refs[3:6], refs[6:9], refs[9]
    copies = [
        pltpu.make_async_copy(
            history_ref.at[u, pl.ds(pl.multiple_of(earlier_rows(len_ref[u]), CHUNK), CHUNK)],
            last_ref.at[u],
            sem_ref.at[u],
        )
        for u in range(history_ref.shape[0])
    ]
    copies += [
        pltpu.make_async_copy(source, target, sem_ref.at[history_ref.shape[0] + k])
        for k, (source, target) in enumerate(zip(weights, targets))
    ]
    for copy in copies:
        copy.start()
    users = history_ref.shape[0]
    for u in range(users):
        live = len_ref[u] - earlier_rows(len_ref[u])
        live_ref[u : u + 1, :] = jnp.full((1, LANES), live, jnp.int32).astype(F32)
        live_ref[users + u : users + u + 1, :] = jnp.full((1, LANES), len_ref[u], jnp.int32).astype(F32)
    place = jnp.transpose(slot_ref[...])[:, 0:1]
    pick_ref[...] = ones_where(place == iota(pick_ref.shape, 1).astype(F32))
    for copy in copies:
        copy.wait()


def in_hbm(x):
    return pltpu.with_memory_space_constraint(x, pltpu.HBM)


def in_vmem(x):
    return pltpu.with_memory_space_constraint(x, pltpu.VMEM)


def window_cost(size):
    return pl.CostEstimate(flops=1 << 30, bytes_accessed=size, transcendentals=0)


def hbm():
    return pl.BlockSpec(memory_space=pltpu.HBM)


def limit(mib):
    return pltpu.CompilerParams(vmem_limit_bytes=mib << 20)


def vmem():
    return pl.BlockSpec(memory_space=pltpu.VMEM)


def local(
    history,
    lengths,
    candidates,
    item_table,
    value_weight,
    click_hidden,
    convert_hidden,
    click_output,
    convert_output,
):
    users, seq, width = history.shape
    cands = candidates.shape[1]
    table_rows, row_width = item_table.shape
    devices = lax.axis_size("gx") * lax.axis_size("gy")
    total = users * cands
    rows = HEADS * cands
    staged = 5 * table_rows // 8
    table = in_hbm(item_table)
    history = in_hbm(history)
    weights = (in_hbm(value_weight), in_hbm(click_hidden), in_hbm(convert_hidden))

    table_start = pl.pallas_call(
        stage_kernel,
        out_shape=pltpu.VMEM((staged, row_width), BF16),
        in_specs=[hbm()],
        out_specs=vmem(),
        scratch_shapes=[pltpu.SemaphoreType.DMA(())],
        cost_estimate=window_cost(2 * table.size),
        compiler_params=limit(2),
        name="stage",
    )(table)
    request, place = pl.pallas_call(
        functools.partial(request_kernel, owners=devices, row_bits=table_rows.bit_length() - 1),
        out_shape=(pltpu.VMEM((devices, LANES), F32), pltpu.VMEM((8, total), F32)),
        in_specs=[hbm()],
        out_specs=(vmem(), vmem()),
        scratch_shapes=[
            pltpu.VMEM(candidates.shape, jnp.int32),
            pltpu.VMEM((total, total), BF16),
            pltpu.SemaphoreType.DMA(()),
        ],
        compiler_params=limit(8),
        name="request",
    )(in_hbm(candidates))
    asked = lax.all_to_all(request, AXES, 0, 0, tiled=True)
    answer = pl.pallas_call(
        answer_kernel,
        out_shape=jax.ShapeDtypeStruct((devices * 16, LANES), BF16),
        in_specs=[vmem(), vmem(), hbm()],
        out_specs=vmem(),
        scratch_shapes=[
            pltpu.VMEM((devices * SLOTS, 256), BF16),
            pltpu.VMEM((devices * SLOTS, 256), BF16),
            pltpu.VMEM((devices * SLOTS, row_width), F32),
            pltpu.VMEM((table_rows - staged, row_width), BF16),
            pltpu.SemaphoreType.DMA(()),
        ],
        compiler_params=limit(24),
        name="answer",
    )(asked, in_vmem(table_start), table)
    answered = lax.all_to_all(answer, AXES, 0, 0, tiled=True)
    prepared = pl.pallas_call(
        prepare_kernel,
        out_shape=(
            pltpu.VMEM((2 * users, LANES), F32),
            pltpu.VMEM((total, devices * SLOTS), BF16),
            pltpu.VMEM((users, CHUNK, width), BF16),
            *(pltpu.VMEM(w.shape, BF16) for w in weights),
        ),
        in_specs=[pl.BlockSpec(memory_space=pltpu.SMEM), vmem()] + [hbm()] * 4,
        out_specs=(vmem(),) * 6,
        scratch_shapes=[pltpu.SemaphoreType.DMA((users + 3,))],
        cost_estimate=window_cost(1 << 22),
        compiler_params=limit(4),
        name="prepare",
    )(lengths, place, history, *weights)
    live, pick, start, *weights = (in_vmem(x) for x in prepared)
    return pl.pallas_call(
        attend_kernel,
        out_shape=(
            jax.ShapeDtypeStruct((users, cands), F32),
            jax.ShapeDtypeStruct((users, cands), F32),
        ),
        in_specs=[vmem()] * 7 + [hbm()] + [vmem()] * 2,
        out_specs=(vmem(), vmem()),
        scratch_shapes=[
            pltpu.VMEM((users, seq - CHUNK, width), BF16),
            pltpu.VMEM((users, rows, width), BF16),
            pltpu.VMEM((total, 3 * width), BF16),
            pltpu.VMEM((users + 1, rows, width), F32),
            pltpu.VMEM((users + 1, rows, LANES), F32),
            pltpu.VMEM((users + 1, rows, LANES), F32),
            *[pltpu.VMEM((rows, CHUNK), F32)] * 2,
            *[pltpu.VMEM((rows, CHUNK), BF16)] * 2,
            *[pltpu.VMEM((rows, LANES), F32)] * 2,
            pltpu.VMEM((2, total, click_hidden.shape[1]), F32),
            pltpu.VMEM((users, rows, CHUNK), F32),
            pltpu.SMEM((users * (seq // CHUNK - 1) + 5,), jnp.int32),
            pltpu.SMEM((users,), jnp.int32),
            pltpu.SemaphoreType.DMA((seq // CHUNK - 1,)),
        ],
        compiler_params=limit(24),
        name="attend",
    )(
        live,
        pick,
        answered,
        start,
        *weights,
        history,
        click_output.reshape(1, -1),
        convert_output.reshape(1, -1),
    )


def solution(mesh):
    split = P(AXES)
    return jax.shard_map(
        local,
        mesh=mesh,
        in_specs=(split, split, split, split, P(), P(), P(), P(), P()),
        out_specs=(split, split),
        check_vma=False,
    )
```
